32 devices in a mesh: dp: 8 (over z, core), ctx: 4 (over y, x).
Axes of the slice: x: 2, y: 2, z: 4, core: 2. Of those that a mesh axis runs over, the one named last changes fastest.
Arguments:
- latents: bfloat16 [2, 8, 2048, 1152], P(None, 'dp', 'ctx'), may hold values from -6 to 6
- condition: bfloat16 [2, 8, 1152], P(None, 'dp'), may hold values from -6 to 6
- cotangent: bfloat16 [2, 8, 2048, 1152], P(None, 'dp', 'ctx'), may hold values from -6 to 6
- ada_weight: bfloat16 [1152, 6912], P('dp'), may hold values from -0.1875 to 0.1875
- ada_bias: bfloat16 [6912], P('dp'), may hold values from -2 to 2
- qkv_weight: bfloat16 [1152, 3456], P('dp'), may hold values from -0.1875 to 0.1875
- query_bias: bfloat16 [1152], P('dp'), may hold values from -2 to 2
- value_bias: bfloat16 [1152], P('dp'), may hold values from -2 to 2
- out_weight: bfloat16 [1152, 1152], P('dp'), may hold values from -1 to 1
- out_bias: bfloat16 [1152], P('dp'), may hold values from -2 to 2
- fc1_weight: bfloat16 [1152, 4608], P('dp'), may hold values from -0.1875 to 0.1875
- fc1_bias: bfloat16 [4608], P('dp'), may hold values from -2 to 2
- fc2_weight: bfloat16 [4608, 1152], P('dp'), may hold values from -0.09375 to 0.09375
- fc2_bias: bfloat16 [1152], P('dp'), may hold values from -2 to 2
Outputs:
- block_out: bfloat16 [2, 8, 2048, 1152], P(None, 'dp', 'ctx')
- grad_latents: float32 [2, 8, 2048, 1152], P(None, 'dp', 'ctx')
- grad_condition: float32 [2, 8, 1152], P(None, 'dp')
- grad_ada_weight: float32 [1152, 6912], P('dp')
- grad_ada_bias: float32 [6912], P('dp')
- grad_qkv_weight: float32 [1152, 3456], P('dp')
- grad_query_bias: float32 [1152], P('dp')
- grad_value_bias: float32 [1152], P('dp')
- grad_out_weight: float32 [1152, 1152], P('dp')
- grad_out_bias: float32 [1152], P('dp')
- grad_fc1_weight: float32 [1152, 4608], P('dp')
- grad_fc1_bias: float32 [4608], P('dp')
- grad_fc2_weight: float32 [4608, 1152], P('dp')
- grad_fc2_bias: float32 [1152], P('dp')
The draws below stay inside these ranges and needn't reach their ends.
All inputs are finite; a program needn't handle non-finite values.
Results may differ from the reference program's by a relative error of at most 0.019.
The reference program's roundings to bfloat16 on the way count: a program that leaves them out, or rounds other values in their place, can miss the bound.
Values may be sent and summed in bfloat16 or wider, within the bound.
A program may use at most 320 MiB of HBM per device.

```python
import jax
import jax.numpy as jnp
from jax import lax

D = 1152
HEADS = 16
HDIM = 72
FF = 4608
LEN = 2048
MB = 2
SAMPLES = 8


def shard_levels(own_key, shape, cuts, smallest, top_value):
    gain, own = 1.0, jax.random.fold_in(own_key, 6)
    for dim, shards_of in cuts:
        heights = jnp.exp(jax.random.uniform(jax.random.fold_in(own, dim), (shards_of,), jnp.float32, smallest / len(cuts), top_value / len(cuts)))
        gain = gain * jnp.repeat(heights, shape[dim] // shards_of).reshape([-1 if axis == dim else 1 for axis in range(len(shape))])
    return gain


def normal_values(stream_key, extent, deviation, reach, cuts=(), held_as=jnp.bfloat16):
    array = deviation * jax.random.normal(stream_key, extent, jnp.float32)
    if cuts:
        array = array * shard_levels(stream_key, extent, cuts, -0.22, 0.18)
    return jnp.clip(array, -reach, reach).astype(held_as)


def setup_inputs(seed: int = 0) -> dict:
    key_of = jax.random.split(jax.random.key(seed), 15)
    latents = normal_values(key_of[0], (MB, SAMPLES, LEN, D), 1.0, 6.0, ((1, 8), (2, 4)))
    condition = normal_values(key_of[1], (MB, SAMPLES, D), 1.0, 6.0, ((1, 8),))
    cotangent = normal_values(key_of[2], (MB, SAMPLES, LEN, D), 1.0, 6.0, ((1, 8), (2, 4)))
    ada_weight = normal_values(key_of[3], (D, 6 * D), D ** -0.5, 0.1875, ((0, 8),))
    ada_bias = normal_values(key_of[4], (6 * D,), 0.3, 2.0, ((0, 8),))
    qkv_weight = normal_values(key_of[5], (D, 3 * D), D ** -0.5, 0.1875, ((0, 8),))
    query_bias = normal_values(key_of[6], (D,), 0.3, 2.0, ((0, 8),))
    value_bias = normal_values(key_of[7], (D,), 0.3, 2.0, ((0, 8),))
    out_weight = normal_values(key_of[8], (D, D), (D // 32) ** -0.5, 1.0, ((0, 8),))
    out_bias = normal_values(key_of[9], (D,), 0.3, 2.0, ((0, 8),))
    fc1_weight = normal_values(key_of[10], (D, FF), D ** -0.5, 0.1875, ((0, 8),))
    fc1_bias = normal_values(key_of[11], (FF,), 0.3, 2.0, ((0, 8),))
    fc2_weight = normal_values(key_of[12], (FF, D), FF ** -0.5, 0.09375, ((0, 8),))
    fc2_bias = normal_values(key_of[13], (D,), 0.3, 2.0, ((0, 8),))
    return {"latents": latents, "condition": condition, "cotangent": cotangent, "ada_weight": ada_weight, "ada_bias": ada_bias, "qkv_weight": qkv_weight, "query_bias": query_bias, "value_bias": value_bias, "out_weight": out_weight, "out_bias": out_bias, "fc1_weight": fc1_weight, "fc1_bias": fc1_bias, "fc2_weight": fc2_weight, "fc2_bias": fc2_bias}


HIGHEST = lax.Precision.HIGHEST
EPSILON = 1e-06

@jax.custom_vjp
def low(v):
    return lax.optimization_barrier(v.astype(jnp.bfloat16)).astype(jnp.float32)

@jax.custom_vjp
def low_back(v):
    return v

def low_keep(v):
    return (low(v), None)

def low_pass(kept, grad):
    return (grad,)

def back_keep(v):
    return (v, None)

def back_low(kept, grad):
    return (low(grad),)
low.defvjp(low_keep, low_pass)
low_back.defvjp(back_keep, back_low)

def layer_norm(values):
    centre = lax.optimization_barrier(jnp.mean(values, -1, keepdims=True))
    centred = values - centre
    spread = lax.optimization_barrier(jnp.mean(centred * centred, -1, keepdims=True))
    return centred * lax.rsqrt(spread + EPSILON)

def attention(queries, keys_all, values_all):
    length = queries.shape[0]
    block = min(512, length)
    scaling = HDIM ** (-0.5)
    key_heads = keys_all.reshape(length, HEADS, HDIM)
    value_heads = values_all.reshape(length, HEADS, HDIM)

    def one_block(query_block):
        scores = jnp.einsum('qhd,khd->hqk', query_block, key_heads, precision=HIGHEST) * scaling
        scores = low_back(scores)
        probs = low(jax.nn.softmax(scores, axis=-1))
        return jnp.einsum('hqk,khd->qhd', probs, value_heads, precision=HIGHEST)
    blocks = lax.map(jax.checkpoint(one_block), queries.reshape(length // block, block, HEADS, HDIM))
    return blocks.reshape(length, HEADS * HDIM)

def forward(latent, cond, params):
    ada_w, ada_b, qkv_w, query_b, value_b, out_w, out_b, fc1_w, fc1_b, fc2_w, fc2_b = params
    modulation = jnp.dot(low(jax.nn.silu(cond)), ada_w, precision=HIGHEST) + ada_b
    modulation = low_back(modulation)
    shift_one, scale_one, gate_one, shift_two, scale_two, gate_two = jnp.split(modulation, 6)
    mixed_one = low(layer_norm(latent) * (1.0 + scale_one) + shift_one)
    projected = jnp.dot(mixed_one, qkv_w, precision=HIGHEST)
    queries = low(low_back(projected[:, :D] + query_b))
    keys_all = low(low_back(projected[:, D:2 * D]))
    values_all = low(low_back(projected[:, 2 * D:] + value_b))
    attended = low(low_back(attention(queries, keys_all, values_all)))
    branch_one = low_back(jnp.dot(attended, out_w, precision=HIGHEST) + out_b)
    middle = latent + gate_one * branch_one
    mixed_two = low(layer_norm(middle) * (1.0 + scale_two) + shift_two)
    pre_act = low_back(jnp.dot(mixed_two, fc1_w, precision=HIGHEST) + fc1_b)
    hidden = low(jax.nn.gelu(pre_act, approximate=True))
    branch_two = low_back(jnp.dot(hidden, fc2_w, precision=HIGHEST) + fc2_b)
    return middle + gate_two * branch_two

def reference(latents, condition, cotangent, ada_weight, ada_bias, qkv_weight, query_bias, value_bias, out_weight, out_bias, fc1_weight, fc1_bias, fc2_weight, fc2_bias):
    params = tuple((p.astype(jnp.float32) for p in (ada_weight, ada_bias, qkv_weight, query_bias, value_bias, out_weight, out_bias, fc1_weight, fc1_bias, fc2_weight, fc2_bias)))
    count = MB * SAMPLES
    flat_latents = latents.astype(jnp.float32).reshape(count, LEN, D)
    flat_conds = condition.astype(jnp.float32).reshape(count, D)
    flat_cots = cotangent.astype(jnp.float32).reshape(count, LEN, D)

    def one_latent(totals, items):
        latent, cond, upstream = items
        result, pull = jax.vjp(forward, latent, cond, params)
        d_latent, d_cond, d_params = pull(upstream)
        totals = jax.tree.map(lambda a, b: a + b, totals, d_params)
        return (totals, (result, d_latent, d_cond))
    zeros = jax.tree.map(jnp.zeros_like, params)
    totals, (results, d_latents, d_conds) = lax.scan(one_latent, zeros, (flat_latents, flat_conds, flat_cots))
    block_out = results.reshape(MB, SAMPLES, LEN, D).astype(jnp.bfloat16)
    grad_latents = d_latents.reshape(MB, SAMPLES, LEN, D)
    grad_condition = d_conds.reshape(MB, SAMPLES, D)
    return (block_out, grad_latents, grad_condition, totals[0], totals[1], totals[2], totals[3], totals[4], totals[5], totals[6], totals[7], totals[8], totals[9], totals[10])
```

```python
from functools import partial

import jax
import jax.numpy as jnp
from jax import lax
from jax.experimental import pallas as pl
from jax.experimental.pallas import tpu as pltpu
from jax.sharding import PartitionSpec as P

D = 1152
HEADS = 16
HDIM = 72
FF = 4608
PAIR = 2 * HDIM
EPSILON = 1e-06
LOG2E = 1.4426950408889634
SOFT = HDIM**-0.5 * LOG2E
BOTH = ("dp", "ctx")

f32 = jnp.float32
bf16 = jnp.bfloat16


def contract(a, b, ca, cb):
    return lax.dot_general(a, b, (((ca,), (cb,)), ((), ())), preferred_element_type=f32)


def norm_rows(values):
    centre = jnp.mean(values, -1, keepdims=True)
    centred = values - centre
    spread = jnp.mean(centred * centred, -1, keepdims=True)
    inverse = lax.rsqrt(spread + EPSILON)
    return (centred * inverse, inverse)


def norm_back(grad_hat, normed, inverse):
    first = jnp.mean(grad_hat, -1, keepdims=True)
    second = jnp.mean(grad_hat * normed, -1, keepdims=True)
    return inverse * (grad_hat - first - normed * second)


def attend_kernel(parts, block, q_ref, *refs):
    k_refs, v_refs = refs[:parts], refs[parts : 2 * parts]
    o_ref, lse_ref = refs[2 * parts :]
    for h in range(2):
        rows = slice(h * HDIM, (h + 1) * HDIM)
        keys = [k[rows, :] for k in k_refs]
        values = [v[rows, :].T for v in v_refs]
        for i in range(q_ref.shape[1] // block):
            cols = slice(i * block, (i + 1) * block)
            q = q_ref[rows, cols].T
            scores = [contract(q, k, 1, 0) for k in keys]
            top = jnp.max(scores[0], -1, keepdims=True)
            for s in scores[1:]:
                top = jnp.maximum(top, jnp.max(s, -1, keepdims=True))
            total, out = 0.0, 0.0
            for s, v in zip(scores, values):
                e = jnp.exp2((s - top) * SOFT)
                total = total + jnp.sum(e, -1, keepdims=True)
                out = out + contract(e.astype(bf16), v, 1, 0)
            o_ref[rows, cols] = (out / total).T.astype(bf16)
            lse_ref[0, h : h + 1, cols] = (top * SOFT + jnp.log2(total)).T


def attend(qkv, others):
    tokens = qkv.shape[1]
    parts = 1 + len(others)
    pairs = HEADS // 2
    block = min(256, tokens)

    def at(offset):
        return pl.BlockSpec((PAIR, tokens), lambda i: (i + offset, 0))

    ops = tokens * tokens * parts * HEADS
    return pl.pallas_call(
        partial(attend_kernel, parts, block),
        grid=(pairs,),
        in_specs=[at(0), at(pairs)]
        + [at(0) for _ in others]
        + [at(2 * pairs)]
        + [at(pairs) for _ in others],
        out_specs=[at(0), pl.BlockSpec((1, 2, tokens), lambda i: (i, 0, 0))],
        out_shape=[
            jax.ShapeDtypeStruct((D, tokens), bf16),
            jax.ShapeDtypeStruct((pairs, 2, tokens), f32),
        ],
        cost_estimate=pl.CostEstimate(
            flops=4 * ops * 256, bytes_accessed=2 * D * tokens * (2 + 2 * parts), transcendentals=ops
        ),
        compiler_params=pltpu.CompilerParams(vmem_limit_bytes=48 * 2**20),
        name="attend",
    )(qkv, qkv, *others, qkv, *others)


def attend_back_kernel(parts, bq, bk, q_ref, o_ref, do_ref, lse_ref, *refs):
    k_refs, v_refs = refs[:parts], refs[parts : 2 * parts]
    dq_ref, dkv_refs = refs[2 * parts], refs[2 * parts + 1 : 3 * parts + 1]
    dk_acc, dv_acc = refs[3 * parts + 1 :]
    tokens = q_ref.shape[1]
    for h in range(2):
        rows = slice(h * HDIM, (h + 1) * HDIM)
        qt, dot = q_ref[rows, :], do_ref[rows, :]
        q, do = qt.T, dot.T
        inner = jnp.sum(dot.astype(f32) * o_ref[rows, :].astype(f32), 0, keepdims=True).T
        lse = lse_ref[0, h : h + 1, :].T
        kts = [k[rows, :] for k in k_refs]
        vts = [v[rows, :] for v in v_refs]
        ks = [k.T for k in kts]
        for i in range(tokens // bq):
            qs = slice(i * bq, (i + 1) * bq)
            dq = 0.0
            for part in range(parts):
                for j in range(tokens // bk):
                    cols = slice(j * bk, (j + 1) * bk)
                    p = jnp.exp2(contract(q[qs], kts[part][:, cols], 1, 0) * SOFT - lse[qs])
                    d_probs = contract(do[qs], vts[part][:, cols], 1, 0)
                    ds = (p * (d_probs - inner[qs])).astype(bf16)
                    dv = contract(dot[:, qs], p.astype(bf16), 1, 0)
                    dk = contract(qt[:, qs], ds, 1, 0)
                    dq = dq + contract(ds, ks[part][cols], 1, 0)
                    if i == 0:
                        dv_acc[part, :, cols] = dv
                        dk_acc[part, :, cols] = dk
                    else:
                        dv_acc[part, :, cols] += dv
                        dk_acc[part, :, cols] += dk
            dq_ref[rows, qs] = (dq.T * HDIM**-0.5).astype(bf16)
        for part in range(parts):
            dkv_refs[part][0, rows, :] = (dk_acc[part] * HDIM**-0.5).astype(bf16)
            dkv_refs[part][1, rows, :] = dv_acc[part].astype(bf16)


def attend_back(qkv, others, attended, d_attended, lse):
    tokens = qkv.shape[1]
    parts = 1 + len(others)
    pairs = HEADS // 2
    block = min(512, tokens)

    def at(offset):
        return pl.BlockSpec((PAIR, tokens), lambda i: (i + offset, 0))

    both = pl.BlockSpec((2, PAIR, tokens), lambda i: (0, i, 0))
    ops = tokens * tokens * parts * HEADS
    return pl.pallas_call(
        partial(attend_back_kernel, parts, block, block),
        grid=(pairs,),
        in_specs=[at(0), at(0), at(0), pl.BlockSpec((1, 2, tokens), lambda i: (i, 0, 0)), at(pairs)]
        + [at(0) for _ in others]
        + [at(2 * pairs)]
        + [at(pairs) for _ in others],
        out_specs=[at(0)] + [both] * parts,
        out_shape=[jax.ShapeDtypeStruct((D, tokens), bf16)]
        + [jax.ShapeDtypeStruct((2, D, tokens), bf16)] * parts,
        scratch_shapes=[pltpu.VMEM((parts, HDIM, tokens), f32)] * 2,
        cost_estimate=pl.CostEstimate(
            flops=10 * ops * 256, bytes_accessed=2 * D * tokens * (4 + 4 * parts), transcendentals=ops
        ),
        compiler_params=pltpu.CompilerParams(vmem_limit_bytes=48 * 2**20),
        name="attend_back",
    )(qkv, attended, d_attended, lse, qkv, *others, qkv, *others)


def ring(value, axis, size, step):
    return lax.ppermute(value, axis, [(i, (i + step) % size) for i in range(size)])


def gather_small(value, axis, size, step=1):
    count = size // step
    me = lax.axis_index(axis) // step
    came = [value] + [ring(value, axis, size, step * r) for r in range(1, count)]
    back = jnp.stack(came[::-1])
    return lax.dynamic_slice_in_dim(jnp.concatenate([back, back]), count - 1 - me, count)


def swap_cores(value, dp):
    return lax.ppermute(value, "dp", [(i, i ^ 1) for i in range(dp)])


def move_maps(dp, ctx, micro):
    per_latent = ctx // micro
    maps = []
    for r in range(micro):
        pairs = []
        for plane in range(dp // 2):
            for core in range(2):
                for c in range(ctx):
                    latent = ((c + r) % micro) * 2 + core
                    place = latent * per_latent + c // micro
                    target = (plane * 2 + place % 2) * ctx + place // 2
                    pairs.append(((plane * 2 + core) * ctx + c, target))
        maps.append(pairs)
    return maps


def peer_maps(dp, ctx, micro):
    per_latent = ctx // micro
    maps = []
    for r in range(1, per_latent):
        pairs = []
        for plane in range(dp // 2):
            for place in range(2 * ctx):
                other = place // per_latent * per_latent + (place + r) % per_latent
                pairs.append(
                    (
                        (plane * 2 + place % 2) * ctx + place // 2,
                        (plane * 2 + other % 2) * ctx + other // 2,
                    )
                )
        maps.append(pairs)
    return maps


def inverse(pairs):
    return [(b, a) for a, b in pairs]


def local(
    latents,
    condition,
    cotangent,
    ada_weight,
    ada_bias,
    qkv_weight,
    query_bias,
    value_bias,
    out_weight,
    out_bias,
    fc1_weight,
    fc1_bias,
    fc2_weight,
    fc2_bias,
    *,
    dp,
    ctx,
):
    micro, _, length, _ = latents.shape
    planes = dp // 2
    rows = D // dp
    fast = ctx == 4 and dp == 8 and micro == 2
    per_latent = ctx // micro
    me_dp = lax.axis_index("dp")
    me_ctx = lax.axis_index("ctx")
    core = me_dp % 2
    moves = move_maps(dp, ctx, micro)
    peers = peer_maps(dp, ctx, micro)
    my_latent = me_ctx * 2 // per_latent
    my_micro, my_side = my_latent // 2, my_latent % 2

    def bring(value):
        came = []
        for r in range(micro):
            block = lax.dynamic_index_in_dim(value, (me_ctx + r) % micro, 0, keepdims=False)[0]
            came.append(lax.ppermute(block, BOTH, moves[r]))
        return jnp.concatenate(came, 0)

    def send_home(value):
        came = jnp.stack(
            [
                lax.ppermute(value[r * length : (r + 1) * length], BOTH, inverse(moves[r]))
                for r in range(micro)
            ]
        )
        return jnp.stack(
            [
                lax.dynamic_index_in_dim(came, (m - me_ctx) % micro, 0, keepdims=False)
                for m in range(micro)
            ]
        )[:, None]

    qkv_w = lax.all_gather(qkv_weight, "dp", axis=0, tiled=True)
    out_w = lax.all_gather(out_weight, "dp", axis=0, tiled=True)
    fc1_w = lax.all_gather(fc1_weight, "dp", axis=0, tiled=True)
    fc2_w = lax.all_gather(fc2_weight, "dp", axis=0, tiled=True)

    small = jnp.concatenate(
        [condition[:, 0].reshape(micro * D), query_bias, value_bias, out_bias, fc1_bias, fc2_bias]
    )
    small_all = gather_small(small, "dp", dp)
    cond_all = small_all[:, : micro * D].reshape(dp, micro, D)
    bias_all = small_all[:, micro * D :].astype(f32)
    query_b = bias_all[:, :rows].reshape(D)
    value_b = bias_all[:, rows : 2 * rows].reshape(D)
    out_b = bias_all[:, 2 * rows : 3 * rows].reshape(D)
    fc1_b = bias_all[:, 3 * rows : 3 * rows + FF // dp].reshape(FF)
    fc2_b = bias_all[:, 3 * rows + FF // dp :].reshape(D)

    x_low = bring(latents)
    upstream_low = bring(cotangent)
    tokens = x_low.shape[0]

    act_rows = jax.nn.silu(
        lax.dynamic_slice_in_dim(cond_all, me_dp * rows, rows, 2).astype(f32)
    ).astype(bf16)
    act_rows = act_rows.reshape(planes, 2, micro, rows).transpose(0, 2, 1, 3)
    act_mine = lax.dynamic_index_in_dim(
        act_rows.reshape(planes, micro * 2, rows), my_latent, 1, keepdims=False
    )
    partial_mod = jnp.dot(act_mine, ada_weight, preferred_element_type=f32)
    own_bias = lax.dynamic_update_slice_in_dim(
        jnp.zeros((6 * D,), f32), ada_bias.astype(f32), me_dp * (6 * D // dp), 0
    )
    partial_mod = partial_mod + own_bias
    modul = 0.0
    for r in range(dp):
        row = lax.dynamic_index_in_dim(partial_mod, (me_dp + r) % dp // 2, 0, keepdims=False)
        modul = modul + (ring(row, "dp", dp, r) if r else row)
    shift_one, scale_one, gate_one, shift_two, scale_two, gate_two = [
        modul[part * D : (part + 1) * D] for part in range(6)
    ]

    inputs = x_low.astype(f32)
    normed_one, inverse_one = norm_rows(inputs)
    mixed_one = (normed_one * (1.0 + scale_one) + shift_one).astype(bf16)
    qkv_bias = jnp.concatenate([query_b, jnp.zeros((D,), f32), value_b])
    qkv = (contract(qkv_w, mixed_one, 0, 1) + qkv_bias[:, None]).astype(bf16)
    others = [lax.ppermute(qkv[D:], BOTH, peer) for peer in peers]
    attended, lse = attend(qkv, others)
    branch_one = contract(attended, out_w, 0, 0) + out_b
    middle = inputs + gate_one * branch_one
    normed_two, inverse_two = norm_rows(middle)
    mixed_two = (normed_two * (1.0 + scale_two) + shift_two).astype(bf16)
    pre_act = jnp.dot(mixed_two, fc1_w, preferred_element_type=f32) + fc1_b
    hidden, gelu_pull = jax.vjp(partial(jax.nn.gelu, approximate=True), pre_act)
    hidden_low = hidden.astype(bf16)
    branch_two = jnp.dot(hidden_low, fc2_w, preferred_element_type=f32) + fc2_b
    block_out = send_home((middle + gate_two * branch_two).astype(bf16))

    def halves(values):
        width = values.shape[1] // 2
        return (
            lax.dynamic_slice_in_dim(values, core * width, width, 1),
            lax.dynamic_slice_in_dim(values, (1 - core) * width, width, 1),
        )

    def chip_sum(values, grads, dim):
        keep, give = halves(values)
        came = swap_cores(contract(give, grads, 0, dim).astype(bf16), dp)
        return (contract(keep, grads, 0, dim) + came.astype(f32)).astype(bf16)

    def plane_sum(pick):
        total = pick(me_ctx).astype(f32)
        for r in range(1, 4):
            moved = lax.ppermute(pick(me_ctx ^ r), "ctx", [(i, i ^ r) for i in range(4)])
            total = total + moved.astype(f32)
        return total.astype(bf16)

    def line_sum(block):
        total = 0.0
        for r in range(4):
            piece = lax.dynamic_index_in_dim(block, (me_dp // 2 + r) % 4, 0, keepdims=False)
            pairs = [(i, 4 * (i % 2) + (i // 2 + r) % 4) for i in range(8)]
            total = total + lax.ppermute(piece, "dp", pairs).astype(f32)
        return total.astype(bf16)

    def share(block):
        came = [block] + [
            lax.ppermute(block, "ctx", [(i, i ^ r) for i in range(4)]) for r in range(1, 4)
        ]
        stack = jnp.stack(came)
        return [
            lax.dynamic_index_in_dim(stack, me_ctx ^ j, 0, keepdims=False).astype(f32)
            for j in range(4)
        ]

    def slow_sum(values, grads, dim):
        total = contract(values, grads, 0, dim).astype(bf16)
        total = lax.psum_scatter(total, "dp", scatter_dimension=0, tiled=True)
        return lax.psum(total, "ctx").astype(f32)

    upstream = upstream_low.astype(f32)
    d_gate_two = jnp.sum(branch_two * upstream, 0)
    d_branch_two = (gate_two * upstream).astype(bf16)
    sum_fc2_b = jnp.sum(d_branch_two.astype(f32), 0)
    d_hidden = contract(d_branch_two, fc2_w, 1, 1)
    d_pre = gelu_pull(d_hidden)[0].astype(bf16)
    sum_fc1_b = jnp.sum(d_pre.astype(f32), 0)
    d_mixed_two = contract(d_pre, fc1_w, 1, 1)
    d_shift_two = jnp.sum(d_mixed_two, 0)
    d_scale_two = jnp.sum(d_mixed_two * normed_two, 0)
    d_middle = upstream + norm_back(d_mixed_two * (1.0 + scale_two), normed_two, inverse_two)
    d_gate_one = jnp.sum(branch_one * d_middle, 0)
    d_branch_one = (gate_one * d_middle).astype(bf16)
    sum_out_b = jnp.sum(d_branch_one.astype(f32), 0)
    d_attended = contract(out_w, d_branch_one, 1, 1).astype(bf16)

    if fast:
        chip_fc2 = chip_sum(hidden_low, d_branch_two, 0).reshape(4, 4, rows, D)
        chip_fc1 = chip_sum(mixed_two, d_pre, 0)
        plane_fc2 = plane_sum(
            lambda j: lax.dynamic_index_in_dim(chip_fc2, j, 1, keepdims=False)
        )
        plane_fc1 = plane_sum(
            lambda j: lax.dynamic_slice_in_dim(chip_fc1, j * D, D, 1).reshape(4, rows, D)
        )
        shared = share(line_sum(jnp.stack([plane_fc2, plane_fc1], 1)))
        grad_fc2_w = jnp.concatenate([s[0] for s in shared], 0)
        grad_fc1_w = jnp.concatenate([s[1] for s in shared], 1)
        chip_out = chip_sum(attended.T, d_branch_one, 0)
    else:
        grad_fc2_w = slow_sum(hidden_low, d_branch_two, 0)
        grad_fc1_w = slow_sum(mixed_two, d_pre, 0)
        grad_out_w = slow_sum(attended.T, d_branch_one, 0)

    d_query, d_own, *d_others = attend_back(qkv, others, attended, d_attended, lse)
    d_kv = d_own.astype(f32)
    for peer, value in zip(peers, d_others):
        d_kv = d_kv + lax.ppermute(value, BOTH, inverse(peer)).astype(f32)
    d_qkv = jnp.concatenate([d_query, d_kv.astype(bf16).reshape(2 * D, tokens)], 0)
    sum_qkv_b = jnp.sum(d_qkv.astype(f32), 1)
    d_mixed_one = contract(d_qkv, qkv_w, 0, 1)
    d_shift_one = jnp.sum(d_mixed_one, 0)
    d_scale_one = jnp.sum(d_mixed_one * normed_one, 0)
    d_inputs = d_middle + norm_back(d_mixed_one * (1.0 + scale_one), normed_one, inverse_one)
    grad_latents = send_home(d_inputs.astype(bf16)).astype(f32)

    if fast:
        chip_qkv = chip_sum(mixed_one, d_qkv, 1)
        chip_attn = jnp.concatenate([chip_qkv, chip_out], 1)
        plane_attn = plane_sum(
            lambda j: lax.dynamic_slice_in_dim(chip_attn, j * D, D, 1).reshape(4, rows, D)
        )
        shared = share(line_sum(plane_attn))
        grad_qkv_w = jnp.concatenate(shared[:3], 1)
        grad_out_w = shared[3]
    else:
        grad_qkv_w = slow_sum(mixed_one, d_qkv, 1)

    vector = jnp.concatenate(
        [d_shift_one, d_scale_one, d_gate_one, d_shift_two, d_scale_two, d_gate_two]
        + [sum_qkv_b[:D], sum_qkv_b[2 * D :], sum_out_b, sum_fc1_b, sum_fc2_b]
    )
    vector = vector + swap_cores(vector, dp)
    chips = gather_small(vector, "ctx", ctx)
    lats = micro * 2
    d_mods = jnp.sum(chips[:, : 6 * D].reshape(lats, ctx // lats, 6 * D), 1)
    packed = jnp.concatenate(
        [d_mods.reshape(lats * 6 * D), jnp.sum(chips[:, 6 * D :], 0)]
    ).astype(bf16)
    packed = gather_small(packed, "dp", dp, 2)
    d_modul = packed[:, : lats * 6 * D].reshape(planes, lats, 6 * D)
    bias_sums = jnp.sum(packed[:, lats * 6 * D :].astype(f32), 0)

    def owned(start, width):
        return lax.dynamic_slice_in_dim(bias_sums, start + me_dp * (width // dp), width // dp)

    grad_query_b = owned(0, D)
    grad_value_b = owned(D, D)
    grad_out_b = owned(2 * D, D)
    grad_fc1_b = owned(3 * D, FF)
    grad_fc2_b = owned(3 * D + FF, D)
    flat_modul = d_modul.reshape(planes * lats, 6 * D)
    grad_ada_w = contract(act_rows.reshape(planes * lats, rows), flat_modul, 0, 0)
    grad_ada_b = lax.dynamic_slice_in_dim(
        jnp.sum(flat_modul.astype(f32), 0), me_dp * (6 * D // dp), 6 * D // dp
    )
    d_act = contract(flat_modul, ada_weight, 1, 1)
    d_act = d_act.reshape(planes, micro, 2, rows).transpose(0, 2, 1, 3).reshape(dp, micro, rows)
    came = []
    for r in range(dp):
        piece = lax.dynamic_index_in_dim(d_act, (me_dp + r) % dp, 0, keepdims=False)
        came.append(ring(piece, "dp", dp, r) if r else piece)
    back = jnp.stack(came[::-1])
    d_cond = lax.dynamic_slice_in_dim(jnp.concatenate([back, back]), dp - 1 - me_dp, dp)
    d_cond = d_cond.transpose(1, 0, 2).reshape(micro, D)
    cond_f = condition[:, 0].astype(f32)
    gate = 1.0 / (1.0 + jnp.exp(-cond_f))
    grad_condition = (d_cond * gate * (1.0 + cond_f * (1.0 - gate)))[:, None]

    return (
        block_out,
        grad_latents,
        grad_condition,
        grad_ada_w,
        grad_ada_b,
        grad_qkv_w,
        grad_query_b,
        grad_value_b,
        grad_out_w,
        grad_out_b,
        grad_fc1_w,
        grad_fc1_b,
        grad_fc2_w,
        grad_fc2_b,
    )


def solution(mesh):
    token = P(None, "dp", "ctx", None)
    line = P(None, "dp", None)
    wide, flat = P("dp", None), P("dp")
    weights = (wide, flat, wide, flat, flat, wide, flat, wide, flat, wide, flat)
    return jax.shard_map(
        partial(local, dp=mesh.shape["dp"], ctx=mesh.shape["ctx"]),
        mesh=mesh,
        in_specs=(token, line, token) + weights,
        out_specs=(token, token, line) + weights,
        check_vma=False,
    )
```

```python
from functools import partial

import jax
import jax.numpy as jnp
from jax import lax
from jax.experimental import pallas as pl
from jax.experimental.pallas import tpu as pltpu
from jax.sharding import PartitionSpec as P


D = 1152
HEADS = 16
HDIM = 72
FF = 4608
PAIR = 2 * HDIM
EPSILON = 1e-06
LOG2E = 1.4426950408889634
SOFT = HDIM**-0.5 * LOG2E
BOTH = ("dp", "ctx")

f32 = jnp.float32
bf16 = jnp.bfloat16


def contract(a, b, ca, cb):
    return lax.dot_general(a, b, (((ca,), (cb,)), ((), ())), preferred_element_type=f32)


def norm_rows(values):
    centre = jnp.mean(values, -1, keepdims=True)
    centred = values - centre
    spread = jnp.mean(centred * centred, -1, keepdims=True)
    inverse = lax.rsqrt(spread + EPSILON)
    return (centred * inverse, inverse)


def norm_back(grad_hat, normed, inverse):
    first = jnp.mean(grad_hat, -1, keepdims=True)
    second = jnp.mean(grad_hat * normed, -1, keepdims=True)
    return inverse * (grad_hat - first - normed * second)


def attend_kernel(parts, block, q_ref, *refs):
    k_refs, v_refs = refs[:parts], refs[parts : 2 * parts]
    o_ref, lse_ref = refs[2 * parts :]
    for h in range(2):
        rows = slice(h * HDIM, (h + 1) * HDIM)
        keys = [k[rows, :] for k in k_refs]
        values = [v[rows, :].T for v in v_refs]
        for i in range(q_ref.shape[1] // block):
            cols = slice(i * block, (i + 1) * block)
            q = q_ref[rows, cols].T
            scores = [contract(q, k, 1, 0) for k in keys]
            top = jnp.max(scores[0], -1, keepdims=True)
            for s in scores[1:]:
                top = jnp.maximum(top, jnp.max(s, -1, keepdims=True))
            total, out = 0.0, 0.0
            for s, v in zip(scores, values):
                e = jnp.exp2((s - top) * SOFT)
                total = total + jnp.sum(e, -1, keepdims=True)
                out = out + contract(e.astype(bf16), v, 1, 0)
            o_ref[rows, cols] = (out / total).T.astype(bf16)
            lse_ref[0, h : h + 1, cols] = (top * SOFT + jnp.log2(total)).T


def attend(qkv, others):
    tokens = qkv.shape[1]
    parts = 1 + len(others)
    pairs = HEADS // 2
    block = min(256, tokens)

    def at(offset):
        return pl.BlockSpec((PAIR, tokens), lambda i: (i + offset, 0))

    ops = tokens * tokens * parts * HEADS
    return pl.pallas_call(
        partial(attend_kernel, parts, block),
        grid=(pairs,),
        in_specs=[at(0), at(pairs)]
        + [at(0) for _ in others]
        + [at(2 * pairs)]
        + [at(pairs) for _ in others],
        out_specs=[at(0), pl.BlockSpec((1, 2, tokens), lambda i: (i, 0, 0))],
        out_shape=[
            jax.ShapeDtypeStruct((D, tokens), bf16),
            jax.ShapeDtypeStruct((pairs, 2, tokens), f32),
        ],
        cost_estimate=pl.CostEstimate(
            flops=4 * ops * 256, bytes_accessed=2 * D * tokens * (2 + 2 * parts), transcendentals=ops
        ),
        compiler_params=pltpu.CompilerParams(vmem_limit_bytes=48 * 2**20),
        name="attend",
    )(qkv, qkv, *others, qkv, *others)


def attend_back_kernel(parts, bq, bk, q_ref, o_ref, do_ref, lse_ref, *refs):
    k_refs, v_refs = refs[:parts], refs[parts : 2 * parts]
    dq_ref, dkv_refs = refs[2 * parts], refs[2 * parts + 1 : 3 * parts + 1]
    dk_acc, dv_acc = refs[3 * parts + 1 :]
    tokens = q_ref.shape[1]
    for h in range(2):
        rows = slice(h * HDIM, (h + 1) * HDIM)
        qt, dot = q_ref[rows, :], do_ref[rows, :]
        q, do = qt.T, dot.T
        inner = jnp.sum(dot.astype(f32) * o_ref[rows, :].astype(f32), 0, keepdims=True).T
        lse = lse_ref[0, h : h + 1, :].T
        kts = [k[rows, :] for k in k_refs]
        vts = [v[rows, :] for v in v_refs]
        ks = [k.T for k in kts]
        for i in range(tokens // bq):
            qs = slice(i * bq, (i + 1) * bq)
            dq = 0.0
            for part in range(parts):
                for j in range(tokens // bk):
                    cols = slice(j * bk, (j + 1) * bk)
                    p = jnp.exp2(contract(q[qs], kts[part][:, cols], 1, 0) * SOFT - lse[qs])
                    d_probs = contract(do[qs], vts[part][:, cols], 1, 0)
                    ds = (p * (d_probs - inner[qs])).astype(bf16)
                    dv = contract(dot[:, qs], p.astype(bf16), 1, 0)
                    dk = contract(qt[:, qs], ds, 1, 0)
                    dq = dq + contract(ds, ks[part][cols], 1, 0)
                    if i == 0:
                        dv_acc[part, :, cols] = dv
                        dk_acc[part, :, cols] = dk
                    else:
                        dv_acc[part, :, cols] += dv
                        dk_acc[part, :, cols] += dk
            dq_ref[rows, qs] = (dq.T * HDIM**-0.5).astype(bf16)
        for part in range(parts):
            dkv_refs[part][0, rows, :] = (dk_acc[part] * HDIM**-0.5).astype(bf16)
            dkv_refs[part][1, rows, :] = dv_acc[part].astype(bf16)


def attend_back(qkv, others, attended, d_attended, lse, first, count):
    tokens = qkv.shape[1]
    parts = 1 + len(others)
    pairs = HEADS // 2
    block = min(512, tokens)

    def at(offset, start=first):
        return pl.BlockSpec((PAIR, tokens), lambda i: (i + (offset + start), 0))

    both = pl.BlockSpec((2, PAIR, tokens), lambda i: (0, i, 0))
    ops = tokens * tokens * parts * 2 * count
    return pl.pallas_call(
        partial(attend_back_kernel, parts, block, block),
        grid=(count,),
        in_specs=[at(0), at(0), at(0)]
        + [pl.BlockSpec((1, 2, tokens), lambda i: (i + first, 0, 0)), at(pairs)]
        + [at(0) for _ in others]
        + [at(2 * pairs)]
        + [at(pairs) for _ in others],
        out_specs=[at(0, 0)] + [both] * parts,
        out_shape=[jax.ShapeDtypeStruct((PAIR * count, tokens), bf16)]
        + [jax.ShapeDtypeStruct((2, PAIR * count, tokens), bf16)] * parts,
        scratch_shapes=[pltpu.VMEM((parts, HDIM, tokens), f32)] * 2,
        cost_estimate=pl.CostEstimate(
            flops=10 * ops * 256,
            bytes_accessed=2 * PAIR * count * tokens * (4 + 4 * parts),
            transcendentals=ops,
        ),
        compiler_params=pltpu.CompilerParams(vmem_limit_bytes=48 * 2**20),
        name="attend_back",
    )(qkv, attended, d_attended, lse, qkv, *others, qkv, *others)


def ring(value, axis, size, step):
    return lax.ppermute(value, axis, [(i, (i + step) % size) for i in range(size)])


def gather_small(value, axis, size, step=1):
    count = size // step
    me = lax.axis_index(axis) // step
    came = [value] + [ring(value, axis, size, step * r) for r in range(1, count)]
    back = jnp.stack(came[::-1])
    return lax.dynamic_slice_in_dim(jnp.concatenate([back, back]), count - 1 - me, count)


def swap_cores(value, dp):
    return lax.ppermute(value, "dp", [(i, i ^ 1) for i in range(dp)])


def move_maps(dp, ctx, micro):
    per_latent = ctx // micro
    maps = []
    for r in range(micro):
        pairs = []
        for plane in range(dp // 2):
            for core in range(2):
                for c in range(ctx):
                    latent = ((c + r) % micro) * 2 + core
                    place = latent * per_latent + c // micro
                    target = (plane * 2 + place % 2) * ctx + place // 2
                    pairs.append(((plane * 2 + core) * ctx + c, target))
        maps.append(pairs)
    return maps


def peer_maps(dp, ctx, micro):
    per_latent = ctx // micro
    maps = []
    for r in range(1, per_latent):
        pairs = []
        for plane in range(dp // 2):
            for place in range(2 * ctx):
                other = place // per_latent * per_latent + (place + r) % per_latent
                pairs.append(
                    (
                        (plane * 2 + place % 2) * ctx + place // 2,
                        (plane * 2 + other % 2) * ctx + other // 2,
                    )
                )
        maps.append(pairs)
    return maps


def inverse(pairs):
    return [(b, a) for a, b in pairs]


MOD_ROWS = 54
MOD_PAD = 64
BIAS_ROWS = 72
VEC_ROWS = MOD_PAD + BIAS_ROWS
MESH = pl.DeviceIdType.MESH


def finish_kernel(
    g_ref, fx_ref, fy_ref, gl_ref, vec_ref,
    gw_ref, home_ref, mods_ref, bias_ref,
    give, got, line_out, line_in, shared, core_in, plane_in, bias_in,
    send, recv,
):
    rows = gw_ref.shape[0]
    length = home_ref.shape[1]
    me, c = lax.axis_index("dp"), lax.axis_index("ctx")
    z, k = me // 2, me % 2
    y, x = c // 2, c % 2
    peer_x, peer_y, peer_d = y * 2 + 1 - x, (1 - y) * 2 + x, (1 - y) * 2 + 1 - x
    partner = me + 1 - 2 * k

    barrier = pltpu.get_barrier_semaphore()
    greeted = [(z * 2 + (k + a) % 2, (c + b) % 4) for a in range(2) for b in range(4) if a or b]
    greeted += [(((z + a) % 4) * 2 + (k + b) % 2, c)
                for a in range(1, 4) for b in range(2)]
    for device in greeted:
        pl.semaphore_signal(barrier, inc=1, device_id=device, device_id_type=MESH)
    pl.semaphore_wait(barrier, len(greeted))

    def copy(src, dst, index, device):
        return pltpu.make_async_remote_copy(
            src_ref=src, dst_ref=dst, send_sem=send.at[index], recv_sem=recv.at[index],
            device_id=device, device_id_type=MESH,
        )

    def block(q, j):
        cols = pl.ds(pl.multiple_of(j * D, D), D)
        return g_ref[q * rows : (q + 1) * rows, cols].astype(f32)

    def first(q, index):
        ref = fx_ref if q < 2 else fy_ref
        start = (q % 2) * rows
        return ref[index, start : start + rows, :].astype(f32)

    started = []

    to_core = copy(vec_ref, core_in, 0, (partner, c))
    to_core.start()
    started.append(to_core)

    order = (0, 2, 1, 3)
    hops = {}
    for q in order:
        if q < 2:
            give[q] = (block(q, peer_y) + first(q, 1 - y)).astype(bf16)
            hops[q] = copy(give.at[q], got.at[q], 1 + q, (me, peer_y))
        else:
            give[q] = (block(q, peer_x) + first(q, 1 - x)).astype(bf16)
            hops[q] = copy(give.at[q], got.at[q], 1 + q, (me, peer_x))
    for q in order:
        hops[q].start()

    for r in range(2):
        slot = y
        target_c = 2 * k + (y + r) % 2
        target = z * 2 + x
        here = (x == k) & (target_c == c)
        src = gl_ref.at[pl.ds(r * length, length), :]

        @pl.when(here)
        def _():
            home_ref[slot] = gl_ref[r * length : (r + 1) * length, :]

        @pl.when(jnp.logical_not(here))
        def _():
            pltpu.make_async_remote_copy(
                src_ref=src, dst_ref=home_ref.at[slot],
                send_sem=send.at[20 + r], recv_sem=recv.at[20 + slot],
                device_id=(target, target_c), device_id_type=MESH,
            ).start()

    to_core.wait_recv()
    plane_in[c] = vec_ref[...] + core_in[...]
    across = []
    for n, peer in enumerate((peer_x, peer_y, peer_d)):
        across.append(copy(plane_in.at[c], plane_in.at[c], 5 + n, (me, peer)))

    for q in order:
        hops[q].wait_recv()
        index = y if q < 2 else x
        total = block(q, c) + first(q, index) + got[q].astype(f32)
        line_out[q] = total.astype(bf16)
        if q == order[0]:
            for item in across:
                item.start()
        target = 4 * k + q
        here = target == me

        @pl.when(here)
        def _():
            line_in[z] = line_out[q]

        @pl.when(jnp.logical_not(here))
        def _():
            pltpu.make_async_remote_copy(
                src_ref=line_out.at[q], dst_ref=line_in.at[z],
                send_sem=send.at[8 + q], recv_sem=recv.at[8 + z],
                device_id=(target, c), device_id_type=MESH,
            ).start()

    for item in across:
        item.wait_recv()
    for n in range(4):
        mods_ref[z, n] = plane_in[n, :MOD_PAD, :].astype(bf16)
    bias_in[z] = (plane_in[0, MOD_PAD:, :] + plane_in[1, MOD_PAD:, :]) + (
        plane_in[2, MOD_PAD:, :] + plane_in[3, MOD_PAD:, :]
    )

    owner_core = me // 4
    total = None
    for n in range(4):
        here = (z == n) & (k == owner_core)

        @pl.when(jnp.logical_not(here))
        def _():
            pltpu.make_async_remote_copy(
                src_ref=line_in.at[n], dst_ref=line_in.at[n],
                send_sem=send.at[8 + n], recv_sem=recv.at[8 + n],
                device_id=(partner, c), device_id_type=MESH,
            ).wait_recv()

    for n in range(4):
        value = line_in[n].astype(f32)
        total = value if total is None else total + value
    shared[c] = total.astype(bf16)
    far = []
    for n in range(1, 4):
        other = ((z + n) % 4) * 2 + k
        far.append(copy(mods_ref.at[z], mods_ref.at[z], 14 + n, (other, c)))
        far.append(copy(bias_in.at[z], bias_in.at[z], 22 + n, (other, c)))
    for item in far:
        item.start()
    spread = []
    for n, peer in enumerate((peer_x, peer_y, peer_d)):
        spread.append(copy(shared.at[c], shared.at[c], 12 + n, (me, peer)))
    for item in spread:
        item.start()
    for item in far:
        item.wait_recv()
    bias_ref[...] = (bias_in[0] + bias_in[1]) + (bias_in[2] + bias_in[3])
    for item in spread:
        item.wait_recv()
    for j in range(4):
        gw_ref[:, j * D : (j + 1) * D] = shared[j].astype(f32)

    for slot in range(2):
        here = (slot * 2 + k == c) & (y == k)

        @pl.when(jnp.logical_not(here))
        def _():
            pltpu.make_async_remote_copy(
                src_ref=home_ref.at[slot], dst_ref=home_ref.at[slot],
                send_sem=send.at[20 + slot], recv_sem=recv.at[20 + slot],
                device_id=(partner, c), device_id_type=MESH,
            ).wait_recv()

    for r in range(2):
        here = (x == k) & (2 * k + (y + r) % 2 == c)

        @pl.when(jnp.logical_not(here))
        def _():
            pltpu.make_async_remote_copy(
                src_ref=gl_ref.at[pl.ds(r * length, length), :], dst_ref=home_ref.at[0],
                send_sem=send.at[20 + r], recv_sem=recv.at[20],
                device_id=(partner, c), device_id_type=MESH,
            ).wait_send()

    for q in range(4):
        here = 4 * k + q == me

        @pl.when(jnp.logical_not(here))
        def _():
            pltpu.make_async_remote_copy(
                src_ref=line_out.at[q], dst_ref=line_in.at[q],
                send_sem=send.at[8 + q], recv_sem=recv.at[8],
                device_id=(partner, c), device_id_type=MESH,
            ).wait_send()

    for item in started + [hops[q] for q in order] + across + far + spread:
        item.wait_send()


def finish(chip, first_x, first_y, tokens, vector):
    rows = chip.shape[0] // 4
    length = tokens.shape[0] // 2
    vmem = pl.BlockSpec(memory_space=pltpu.VMEM)
    piece = (4, rows, D)
    return pl.pallas_call(
        finish_kernel,
        in_specs=[vmem] * 5,
        out_specs=[vmem] * 4,
        out_shape=[
            jax.ShapeDtypeStruct((rows, 4 * D), f32),
            jax.ShapeDtypeStruct((2, length, D), bf16),
            jax.ShapeDtypeStruct((4, 4, MOD_PAD, 128), bf16),
            jax.ShapeDtypeStruct((BIAS_ROWS, 128), f32),
        ],
        scratch_shapes=[pltpu.VMEM(piece, bf16)] * 5
        + [
            pltpu.VMEM((VEC_ROWS, 128), f32),
            pltpu.VMEM((4, VEC_ROWS, 128), f32),
            pltpu.VMEM((4, BIAS_ROWS, 128), f32),
            pltpu.SemaphoreType.DMA((26,)),
            pltpu.SemaphoreType.DMA((26,)),
        ],
        compiler_params=pltpu.CompilerParams(
            collective_id=1, has_side_effects=True, vmem_limit_bytes=40 * 2**20
        ),
        name="finish",
    )(chip, first_x, first_y, tokens, vector)


def local(
    latents,
    condition,
    cotangent,
    ada_weight,
    ada_bias,
    qkv_weight,
    query_bias,
    value_bias,
    out_weight,
    out_bias,
    fc1_weight,
    fc1_bias,
    fc2_weight,
    fc2_bias,
    *,
    dp,
    ctx,
):
    micro, _, length, _ = latents.shape
    planes = dp // 2
    rows = D // dp
    fast = ctx == 4 and dp == 8 and micro == 2
    per_latent = ctx // micro
    me_dp = lax.axis_index("dp")
    me_ctx = lax.axis_index("ctx")
    core = me_dp % 2
    moves = move_maps(dp, ctx, micro)
    peers = peer_maps(dp, ctx, micro)
    my_latent = me_ctx * 2 // per_latent

    def bring(value):
        came = []
        for r in range(micro):
            block = lax.dynamic_index_in_dim(value, (me_ctx + r) % micro, 0, keepdims=False)[0]
            came.append(lax.ppermute(block, BOTH, moves[r]))
        return jnp.concatenate(came, 0)

    def send_home(value):
        came = jnp.stack(
            [
                lax.ppermute(value[r * length : (r + 1) * length], BOTH, inverse(moves[r]))
                for r in range(micro)
            ]
        )
        return jnp.stack(
            [
                lax.dynamic_index_in_dim(came, (m - me_ctx) % micro, 0, keepdims=False)
                for m in range(micro)
            ]
        )[:, None]

    qkv_w = lax.all_gather(qkv_weight, "dp", axis=0, tiled=True)
    out_w = lax.all_gather(out_weight, "dp", axis=0, tiled=True)
    fc1_w = lax.all_gather(fc1_weight, "dp", axis=0, tiled=True)
    fc2_w = lax.all_gather(fc2_weight, "dp", axis=0, tiled=True)

    small = jnp.concatenate(
        [condition[:, 0].reshape(micro * D), query_bias, value_bias, out_bias, fc1_bias, fc2_bias]
    )
    small_all = gather_small(small, "dp", dp)
    cond_all = small_all[:, : micro * D].reshape(dp, micro, D)
    bias_all = small_all[:, micro * D :].astype(f32)
    query_b = bias_all[:, :rows].reshape(D)
    value_b = bias_all[:, rows : 2 * rows].reshape(D)
    out_b = bias_all[:, 2 * rows : 3 * rows].reshape(D)
    fc1_b = bias_all[:, 3 * rows : 3 * rows + FF // dp].reshape(FF)
    fc2_b = bias_all[:, 3 * rows + FF // dp :].reshape(D)

    x_low = bring(latents)
    upstream_low = bring(cotangent)

    act_rows = jax.nn.silu(
        lax.dynamic_slice_in_dim(cond_all, me_dp * rows, rows, 2).astype(f32)
    ).astype(bf16)
    act_rows = act_rows.reshape(planes, 2, micro, rows).transpose(0, 2, 1, 3)
    act_mine = lax.dynamic_index_in_dim(
        act_rows.reshape(planes, micro * 2, rows), my_latent, 1, keepdims=False
    )
    partial_mod = jnp.dot(act_mine, ada_weight, preferred_element_type=f32)
    own_bias = lax.dynamic_update_slice_in_dim(
        jnp.zeros((6 * D,), f32), ada_bias.astype(f32), me_dp * (6 * D // dp), 0
    )
    partial_mod = partial_mod + own_bias
    modul = 0.0
    for r in range(dp):
        row = lax.dynamic_index_in_dim(partial_mod, (me_dp + r) % dp // 2, 0, keepdims=False)
        modul = modul + (ring(row, "dp", dp, r) if r else row)
    shift_one, scale_one, gate_one, shift_two, scale_two, gate_two = [
        modul[part * D : (part + 1) * D] for part in range(6)
    ]

    inputs = x_low.astype(f32)
    normed_one, inverse_one = norm_rows(inputs)
    mixed_one = (normed_one * (1.0 + scale_one) + shift_one).astype(bf16)
    qkv_bias = jnp.concatenate([query_b, jnp.zeros((D,), f32), value_b])
    qkv = (contract(qkv_w, mixed_one, 0, 1) + qkv_bias[:, None]).astype(bf16)
    others = [lax.ppermute(qkv[D:], BOTH, peer) for peer in peers]
    attended, lse = attend(qkv, others)
    branch_one = contract(attended, out_w, 0, 0) + out_b
    middle = inputs + gate_one * branch_one
    normed_two, inverse_two = norm_rows(middle)
    mixed_two = (normed_two * (1.0 + scale_two) + shift_two).astype(bf16)
    pre_act = jnp.dot(mixed_two, fc1_w, preferred_element_type=f32) + fc1_b
    hidden, gelu_pull = jax.vjp(partial(jax.nn.gelu, approximate=True), pre_act)
    hidden_low = hidden.astype(bf16)
    branch_two = jnp.dot(hidden_low, fc2_w, preferred_element_type=f32) + fc2_b
    block_out = send_home((middle + gate_two * branch_two).astype(bf16))

    side_y, side_x = me_ctx // 2, me_ctx % 2

    def halves(values):
        width = values.shape[1] // 2
        return (
            lax.dynamic_slice_in_dim(values, core * width, width, 1),
            lax.dynamic_slice_in_dim(values, (1 - core) * width, width, 1),
        )

    def give(values, grads, dim):
        return swap_cores(contract(halves(values)[1], grads, 0, dim).astype(bf16), dp)

    def keep(values, grads, dim, came):
        return (contract(halves(values)[0], grads, 0, dim) + came.astype(f32)).astype(bf16)

    def hop(value, bit):
        return lax.ppermute(value, "ctx", [(i, i ^ bit) for i in range(4)])

    def plane_give(pick):
        along_x = jnp.stack([pick(y * 2 + 1 - side_x, 0) for y in range(2)])
        along_y = jnp.stack([pick((1 - side_y) * 2 + x, 1) for x in range(2)])
        return along_x, along_y

    def plane_first(given):
        return hop(given[0], 1), hop(given[1], 2)

    def plane_second(pick, came):
        def term(half, index, j):
            value = lax.dynamic_index_in_dim(came[half], index, 0, keepdims=False)
            return pick(j, half).astype(f32) + value.astype(f32)

        along_y = hop(term(0, 1 - side_y, (1 - side_y) * 2 + side_x).astype(bf16), 2)
        along_x = hop(term(1, 1 - side_x, side_y * 2 + 1 - side_x).astype(bf16), 1)
        return along_y, along_x

    def plane_last(pick, came, more):
        total = []
        for half, index in ((0, side_y), (1, side_x)):
            value = lax.dynamic_index_in_dim(came[half], index, 0, keepdims=False)
            total.append(
                pick(me_ctx, half).astype(f32) + value.astype(f32) + more[half].astype(f32)
            )
        return jnp.concatenate(total, 0).astype(bf16)

    def line_moves(block):
        moved = []
        for r in range(4):
            piece = lax.dynamic_index_in_dim(block, (me_dp // 2 + r) % 4, 0, keepdims=False)
            pairs = [(i, 4 * (i % 2) + (i // 2 + r) % 4) for i in range(8)]
            moved.append(lax.ppermute(piece, "dp", pairs))
        return moved

    def total_of(values):
        return sum(v.astype(f32) for v in values).astype(bf16)

    def share(block):
        return [block] + [hop(block, r) for r in range(1, 4)]

    def in_order(came):
        stack = jnp.stack(came)
        return [
            lax.dynamic_index_in_dim(stack, me_ctx ^ j, 0, keepdims=False).astype(f32)
            for j in range(4)
        ]

    def row_pick(chip):
        return lambda j, half: lax.dynamic_slice(
            chip, (half * 2 * rows, j * D), (2 * rows, D)
        ).reshape(2, rows, D)

    def slow_sum(values, grads, dim):
        total = contract(values, grads, 0, dim).astype(bf16)
        total = lax.psum_scatter(total, "dp", scatter_dimension=0, tiled=True)
        return lax.psum(total, "ctx").astype(f32)

    def tie(*values):
        return lax.optimization_barrier(values)

    upstream = upstream_low.astype(f32)
    d_gate_two = jnp.sum(branch_two * upstream, 0)
    d_branch_two = (gate_two * upstream).astype(bf16)
    sum_fc2_b = jnp.sum(d_branch_two.astype(f32), 0)
    if fast:
        came_fc2 = give(hidden_low, d_branch_two, 0)
    d_hidden = contract(d_branch_two, fc2_w, 1, 1)
    d_pre = gelu_pull(d_hidden)[0].astype(bf16)
    sum_fc1_b = jnp.sum(d_pre.astype(f32), 0)
    if fast:
        came_fc2, d_pre = tie(came_fc2, d_pre)
        chip_fc2 = keep(hidden_low, d_branch_two, 0, came_fc2).reshape(4, 4, rows, D)

        def pick_fc2(j, half):
            return lax.dynamic_index_in_dim(
                chip_fc2[2 * half : 2 * half + 2], j, 1, keepdims=False
            )

        given, d_pre = tie(plane_give(pick_fc2), d_pre)
        first_fc2 = plane_first(given)
        came_fc1 = give(mixed_two, d_pre, 0)
    d_mixed_two = contract(d_pre, fc1_w, 1, 1)
    if fast:
        came_fc1, first_fc2, d_mixed_two = tie(came_fc1, first_fc2, d_mixed_two)
        second_fc2 = plane_second(pick_fc2, first_fc2)
        chip_fc1 = keep(mixed_two, d_pre, 0, came_fc1)
        pick_fc1 = row_pick(chip_fc1)
        given, d_mixed_two = tie(plane_give(pick_fc1), d_mixed_two)
        first_fc1 = plane_first(given)
    d_shift_two = jnp.sum(d_mixed_two, 0)
    d_scale_two = jnp.sum(d_mixed_two * normed_two, 0)
    d_middle = upstream + norm_back(d_mixed_two * (1.0 + scale_two), normed_two, inverse_two)
    d_gate_one = jnp.sum(branch_one * d_middle, 0)
    d_branch_one = (gate_one * d_middle).astype(bf16)
    sum_out_b = jnp.sum(d_branch_one.astype(f32), 0)
    d_attended = contract(out_w, d_branch_one, 1, 1).astype(bf16)
    if fast:
        came_out = give(attended.T, d_branch_one, 0)
        plane_fc2 = plane_last(pick_fc2, first_fc2, second_fc2)

    calls = 4
    count = HEADS // 2 // calls
    d_query, d_key, d_value = [], [], []
    pending = None

    def settle(result):
        d_own, moved = result
        total = d_own.astype(f32)
        for value in moved:
            total = total + value.astype(f32)
        total = total.astype(bf16)
        d_key.append(total[0])
        d_value.append(total[1])

    for call in range(calls):
        d_q, d_own, *d_others = attend_back(
            qkv, others, attended, d_attended, lse, call * count, count
        )
        if fast and call == 0:
            d_q, first_fc1 = tie(d_q, first_fc1)
            second_fc1 = plane_second(pick_fc1, first_fc1)
            chip_out = keep(attended.T, d_branch_one, 0, came_out)
            chip_out, d_attended = tie(chip_out, d_attended)
        elif fast and call == 1:
            d_q, second_fc1 = tie(d_q, second_fc1)
            plane_fc = jnp.stack([plane_fc2, plane_last(pick_fc1, first_fc1, second_fc1)], 1)
            plane_fc, d_attended = tie(plane_fc, d_attended)
            moved_fc = line_moves(plane_fc)
        elif fast and call == 3:
            d_q, moved_fc = tie(d_q, moved_fc)
            shared_fc = share(total_of(moved_fc))
        d_query.append(d_q)
        if call < calls - 1:
            d_others, d_attended = tie(d_others, d_attended)
        moved = [
            lax.ppermute(value, BOTH, inverse(peer)) for peer, value in zip(peers, d_others)
        ]
        if pending is not None:
            settle(pending)
        pending = (d_own, moved)
    settle(pending)
    d_qkv = jnp.concatenate(d_query + d_key + d_value, 0)
    sum_qkv_b = jnp.sum(d_qkv.astype(f32), 1)
    if fast:
        came_qkv = give(mixed_one, d_qkv, 1)
        chip_qkv = keep(mixed_one, d_qkv, 1, came_qkv)
        chip_attn = jnp.concatenate([chip_qkv, chip_out], 1)
        given, d_qkv = tie(plane_give(row_pick(chip_attn)), d_qkv)
        first_attn = plane_first(given)
    d_mixed_one = contract(d_qkv, qkv_w, 0, 1)
    d_shift_one = jnp.sum(d_mixed_one, 0)
    d_scale_one = jnp.sum(d_mixed_one * normed_one, 0)
    d_inputs = d_middle + norm_back(d_mixed_one * (1.0 + scale_one), normed_one, inverse_one)
    mod_sums = jnp.concatenate(
        [d_shift_one, d_scale_one, d_gate_one, d_shift_two, d_scale_two, d_gate_two]
    )
    bias_sums = jnp.concatenate(
        [sum_qkv_b[:D], sum_qkv_b[2 * D :], sum_out_b, sum_fc1_b, sum_fc2_b]
    )
    lats = micro * 2

    if fast:
        vector = jnp.concatenate(
            [mod_sums, jnp.zeros(((MOD_PAD - MOD_ROWS) * 128,), f32), bias_sums]
        ).reshape(VEC_ROWS, 128)
        grad_attn, home, mods, bias_sums = finish(
            chip_attn,
            first_attn[0].reshape(2, 2 * rows, D),
            first_attn[1].reshape(2, 2 * rows, D),
            d_inputs.astype(bf16),
            vector,
        )
        grad_latents = home.astype(f32)[:, None]
        grad_qkv_w, grad_out_w = grad_attn[:, : 3 * D], grad_attn[:, 3 * D :]
        flat_modul = mods[:, :, :MOD_ROWS].reshape(planes * lats, 6 * D)
        bias_sums = bias_sums.reshape(-1)
        shared_fc = in_order(shared_fc)
        grad_fc2_w = jnp.concatenate([v[0] for v in shared_fc], 0)
        grad_fc1_w = jnp.concatenate([v[1] for v in shared_fc], 1)
    else:
        grad_fc2_w = slow_sum(hidden_low, d_branch_two, 0)
        grad_fc1_w = slow_sum(mixed_two, d_pre, 0)
        grad_out_w = slow_sum(attended.T, d_branch_one, 0)
        grad_qkv_w = slow_sum(mixed_one, d_qkv, 1)
        grad_latents = send_home(d_inputs.astype(bf16)).astype(f32)
        vector = jnp.concatenate([mod_sums, bias_sums])
        vector = vector + swap_cores(vector, dp)
        chips = gather_small(vector, "ctx", ctx)
        d_mods = jnp.sum(chips[:, : 6 * D].reshape(lats, ctx // lats, 6 * D), 1)
        packed = jnp.concatenate(
            [d_mods.reshape(lats * 6 * D), jnp.sum(chips[:, 6 * D :], 0)]
        ).astype(bf16)
        packed = gather_small(packed, "dp", dp, 2)
        flat_modul = packed[:, : lats * 6 * D].reshape(planes * lats, 6 * D)
        bias_sums = jnp.sum(packed[:, lats * 6 * D :].astype(f32), 0)

    def owned(start, width):
        return lax.dynamic_slice_in_dim(bias_sums, start + me_dp * (width // dp), width // dp)

    grad_query_b = owned(0, D)
    grad_value_b = owned(D, D)
    grad_out_b = owned(2 * D, D)
    grad_fc1_b = owned(3 * D, FF)
    grad_fc2_b = owned(3 * D + FF, D)
    grad_ada_w = contract(act_rows.reshape(planes * lats, rows), flat_modul, 0, 0)
    grad_ada_b = lax.dynamic_slice_in_dim(
        jnp.sum(flat_modul.astype(f32), 0), me_dp * (6 * D // dp), 6 * D // dp
    )
    d_act = contract(flat_modul, ada_weight, 1, 1)
    d_act = d_act.reshape(planes, micro, 2, rows).transpose(0, 2, 1, 3).reshape(dp, micro, rows)
    came = []
    for r in range(dp):
        piece = lax.dynamic_index_in_dim(d_act, (me_dp + r) % dp, 0, keepdims=False)
        came.append(ring(piece, "dp", dp, r) if r else piece)
    back = jnp.stack(came[::-1])
    d_cond = lax.dynamic_slice_in_dim(jnp.concatenate([back, back]), dp - 1 - me_dp, dp)
    d_cond = d_cond.transpose(1, 0, 2).reshape(micro, D)
    cond_f = condition[:, 0].astype(f32)
    gate = 1.0 / (1.0 + jnp.exp(-cond_f))
    grad_condition = (d_cond * gate * (1.0 + cond_f * (1.0 - gate)))[:, None]

    return (
        block_out,
        grad_latents,
        grad_condition,
        grad_ada_w,
        grad_ada_b,
        grad_qkv_w,
        grad_query_b,
        grad_value_b,
        grad_out_w,
        grad_out_b,
        grad_fc1_w,
        grad_fc1_b,
        grad_fc2_w,
        grad_fc2_b,
    )


def solution(mesh):
    token = P(None, "dp", "ctx", None)
    line = P(None, "dp", None)
    wide, flat = P("dp", None), P("dp")
    weights = (wide, flat, wide, flat, flat, wide, flat, wide, flat, wide, flat)
    return jax.shard_map(
        partial(local, dp=mesh.shape["dp"], ctx=mesh.shape["ctx"]),
        mesh=mesh,
        in_specs=(token, line, token) + weights,
        out_specs=(token, token, line) + weights,
        check_vma=False,
    )
```

```python
from functools import partial

import jax
import jax.numpy as jnp
from jax import lax
from jax.experimental import pallas as pl
from jax.experimental.pallas import tpu as pltpu
from jax.sharding import PartitionSpec as P


D = 1152
HEADS = 16
HDIM = 72
FF = 4608
PAIR = 2 * HDIM
EPSILON = 1e-06
LOG2E = 1.4426950408889634
GELU = (2.0 / 3.141592653589793) ** 0.5
SOFT = HDIM**-0.5 * LOG2E
BOTH = ("dp", "ctx")

f32 = jnp.float32
bf16 = jnp.bfloat16


def contract(a, b, ca, cb):
    return lax.dot_general(a, b, (((ca,), (cb,)), ((), ())), preferred_element_type=f32)


def norm_rows(values):
    centre = jnp.mean(values, -1, keepdims=True)
    centred = values - centre
    spread = jnp.mean(centred * centred, -1, keepdims=True)
    inverse = lax.rsqrt(spread + EPSILON)
    return (centred * inverse, inverse)


def norm_back(grad_hat, normed, inverse):
    first = jnp.mean(grad_hat, -1, keepdims=True)
    second = jnp.mean(grad_hat * normed, -1, keepdims=True)
    return inverse * (grad_hat - first - normed * second)


def gelu_pair(u):
    square = u * u
    bent = jnp.tanh(GELU * u * (1.0 + 0.044715 * square))
    half = 0.5 * (1.0 + bent)
    slope = half + 0.5 * u * (1.0 - bent * bent) * (GELU * (1.0 + 3 * 0.044715 * square))
    return (u * half).astype(bf16), slope.astype(bf16)


def attend_kernel(parts, block, q_ref, *refs):
    k_refs, v_refs = refs[:parts], refs[parts : 2 * parts]
    o_ref, lse_ref = refs[2 * parts :]
    for h in range(2):
        rows = slice(h * HDIM, (h + 1) * HDIM)
        keys = [k[rows, :] for k in k_refs]
        values = [v[rows, :].T for v in v_refs]
        for i in range(q_ref.shape[1] // block):
            cols = slice(i * block, (i + 1) * block)
            q = q_ref[rows, cols].T
            scores = [contract(q, k, 1, 0) for k in keys]
            top = jnp.max(scores[0], -1, keepdims=True)
            for s in scores[1:]:
                top = jnp.maximum(top, jnp.max(s, -1, keepdims=True))
            total, out = 0.0, 0.0
            for s, v in zip(scores, values):
                e = jnp.exp2((s - top) * SOFT)
                total = total + jnp.sum(e, -1, keepdims=True)
                out = out + contract(e.astype(bf16), v, 1, 0)
            o_ref[rows, cols] = (out / total).T.astype(bf16)
            lse_ref[0, h : h + 1, cols] = (top * SOFT + jnp.log2(total)).T


def attend(qkv, others):
    tokens = qkv.shape[1]
    parts = 1 + len(others)
    pairs = HEADS // 2
    block = min(256, tokens)

    def at(offset):
        return pl.BlockSpec((PAIR, tokens), lambda i: (i + offset, 0))

    ops = tokens * tokens * parts * HEADS
    return pl.pallas_call(
        partial(attend_kernel, parts, block),
        grid=(pairs,),
        in_specs=[at(0), at(pairs)]
        + [at(0) for _ in others]
        + [at(2 * pairs)]
        + [at(pairs) for _ in others],
        out_specs=[at(0), pl.BlockSpec((1, 2, tokens), lambda i: (i, 0, 0))],
        out_shape=[
            jax.ShapeDtypeStruct((D, tokens), bf16),
            jax.ShapeDtypeStruct((pairs, 2, tokens), f32),
        ],
        cost_estimate=pl.CostEstimate(
            flops=4 * ops * 256, bytes_accessed=2 * D * tokens * (2 + 2 * parts), transcendentals=ops
        ),
        compiler_params=pltpu.CompilerParams(vmem_limit_bytes=48 * 2**20),
        name="attend",
    )(qkv, qkv, *others, qkv, *others)


def attend_back_kernel(parts, bq, bk, q_ref, o_ref, do_ref, lse_ref, *refs):
    k_refs, v_refs = refs[:parts], refs[parts : 2 * parts]
    dq_ref, dkv_refs = refs[2 * parts], refs[2 * parts + 1 : 3 * parts + 1]
    dk_acc, dv_acc = refs[3 * parts + 1 :]
    tokens = q_ref.shape[1]
    for h in range(2):
        rows = slice(h * HDIM, (h + 1) * HDIM)
        qt, dot = q_ref[rows, :], do_ref[rows, :]
        q, do = qt.T, dot.T
        inner = jnp.sum(dot.astype(f32) * o_ref[rows, :].astype(f32), 0, keepdims=True).T
        lse = lse_ref[0, h : h + 1, :].T
        kts = [k[rows, :] for k in k_refs]
        vts = [v[rows, :] for v in v_refs]
        ks = [k.T for k in kts]
        for i in range(tokens // bq):
            qs = slice(i * bq, (i + 1) * bq)
            dq = 0.0
            for part in range(parts):
                for j in range(tokens // bk):
                    cols = slice(j * bk, (j + 1) * bk)
                    p = jnp.exp2(contract(q[qs], kts[part][:, cols], 1, 0) * SOFT - lse[qs])
                    d_probs = contract(do[qs], vts[part][:, cols], 1, 0)
                    ds = (p * (d_probs - inner[qs])).astype(bf16)
                    dv = contract(dot[:, qs], p.astype(bf16), 1, 0)
                    dk = contract(qt[:, qs], ds, 1, 0)
                    dq = dq + contract(ds, ks[part][cols], 1, 0)
                    if i == 0:
                        dv_acc[part, :, cols] = dv
                        dk_acc[part, :, cols] = dk
                    else:
                        dv_acc[part, :, cols] += dv
                        dk_acc[part, :, cols] += dk
            dq_ref[rows, qs] = (dq.T * HDIM**-0.5).astype(bf16)
        for part in range(parts):
            dkv_refs[part][0, rows, :] = (dk_acc[part] * HDIM**-0.5).astype(bf16)
            dkv_refs[part][1, rows, :] = dv_acc[part].astype(bf16)


def attend_back(qkv, others, attended, d_attended, lse, first, count):
    tokens = qkv.shape[1]
    parts = 1 + len(others)
    pairs = HEADS // 2
    block = min(512, tokens)

    def at(offset, start=first):
        return pl.BlockSpec((PAIR, tokens), lambda i: (i + (offset + start), 0))

    both = pl.BlockSpec((2, PAIR, tokens), lambda i: (0, i, 0))
    ops = tokens * tokens * parts * 2 * count
    return pl.pallas_call(
        partial(attend_back_kernel, parts, block, block),
        grid=(count,),
        in_specs=[at(0), at(0), at(0)]
        + [pl.BlockSpec((1, 2, tokens), lambda i: (i + first, 0, 0)), at(pairs)]
        + [at(0) for _ in others]
        + [at(2 * pairs)]
        + [at(pairs) for _ in others],
        out_specs=[at(0, 0)] + [both] * parts,
        out_shape=[jax.ShapeDtypeStruct((PAIR * count, tokens), bf16)]
        + [jax.ShapeDtypeStruct((2, PAIR * count, tokens), bf16)] * parts,
        scratch_shapes=[pltpu.VMEM((parts, HDIM, tokens), f32)] * 2,
        cost_estimate=pl.CostEstimate(
            flops=10 * ops * 256,
            bytes_accessed=2 * PAIR * count * tokens * (4 + 4 * parts),
            transcendentals=ops,
        ),
        compiler_params=pltpu.CompilerParams(vmem_limit_bytes=48 * 2**20),
        name="attend_back",
    )(qkv, attended, d_attended, lse, qkv, *others, qkv, *others)


def ring(value, axis, size, step):
    return lax.ppermute(value, axis, [(i, (i + step) % size) for i in range(size)])


def gather_small(value, axis, size, step=1):
    count = size // step
    me = lax.axis_index(axis) // step
    came = [value] + [ring(value, axis, size, step * r) for r in range(1, count)]
    back = jnp.stack(came[::-1])
    return lax.dynamic_slice_in_dim(jnp.concatenate([back, back]), count - 1 - me, count)


def swap_cores(value, dp):
    return lax.ppermute(value, "dp", [(i, i ^ 1) for i in range(dp)])


def move_maps(dp, ctx, micro):
    per_latent = ctx // micro
    maps = []
    for r in range(micro):
        pairs = []
        for plane in range(dp // 2):
            for core in range(2):
                for c in range(ctx):
                    latent = ((c + r) % micro) * 2 + core
                    place = latent * per_latent + c // micro
                    target = (plane * 2 + place % 2) * ctx + place // 2
                    pairs.append(((plane * 2 + core) * ctx + c, target))
        maps.append(pairs)
    return maps


def peer_maps(dp, ctx, micro):
    per_latent = ctx // micro
    maps = []
    for r in range(1, per_latent):
        pairs = []
        for plane in range(dp // 2):
            for place in range(2 * ctx):
                other = place // per_latent * per_latent + (place + r) % per_latent
                pairs.append(
                    (
                        (plane * 2 + place % 2) * ctx + place // 2,
                        (plane * 2 + other % 2) * ctx + other // 2,
                    )
                )
        maps.append(pairs)
    return maps


def inverse(pairs):
    return [(b, a) for a, b in pairs]


HALF_ROWS = 8
MESH = pl.DeviceIdType.MESH


def finish_kernel(
    g_ref, fx_ref, fy_ref, gl_ref, vec_ref, ada_ref,
    gq_ref, go_ref, tokens_ref, mods_ref, bias_ref, cond_ref,
    give, got, line_out, line_in, shared, home_ref, core_in, plane_in, bias_in, act_out,
    send, recv,
):
    rows = go_ref.shape[0]
    length = home_ref.shape[1]
    me, c = lax.axis_index("dp"), lax.axis_index("ctx")
    z, k = me // 2, me % 2
    y, x = c // 2, c % 2
    peer_x, peer_y, peer_d = y * 2 + 1 - x, (1 - y) * 2 + x, (1 - y) * 2 + 1 - x
    partner = me + 1 - 2 * k

    greet(z, k, c)

    def copy(src, dst, index, device):
        return pltpu.make_async_remote_copy(
            src_ref=src, dst_ref=dst, send_sem=send.at[index], recv_sem=recv.at[index],
            device_id=device, device_id_type=MESH,
        )

    def block(q, j):
        cols = pl.ds(pl.multiple_of(j * D, D), D)
        return g_ref[q * rows : (q + 1) * rows, cols].astype(f32)

    def first(q, index):
        ref = fx_ref if q < 2 else fy_ref
        start = (q % 2) * rows
        return ref[index, start : start + rows, :].astype(f32)

    started = []

    to_core = copy(vec_ref, core_in, 0, (partner, c))
    to_core.start()
    started.append(to_core)

    order = (0, 2, 1, 3)
    hops = {}
    for q in order:
        if q < 2:
            give[q] = (block(q, peer_y) + first(q, 1 - y)).astype(bf16)
            hops[q] = copy(give.at[q], got.at[q], 1 + q, (me, peer_y))
        else:
            give[q] = (block(q, peer_x) + first(q, 1 - x)).astype(bf16)
            hops[q] = copy(give.at[q], got.at[q], 1 + q, (me, peer_x))
    for q in order:
        hops[q].start()

    for r in range(2):
        slot = y
        target_c = 2 * k + (y + r) % 2
        target = z * 2 + x
        here = (x == k) & (target_c == c)
        src = gl_ref.at[pl.ds(r * length, length), :]

        @pl.when(here)
        def _():
            home_ref[slot] = gl_ref[r * length : (r + 1) * length, :]

        @pl.when(jnp.logical_not(here))
        def _():
            pltpu.make_async_remote_copy(
                src_ref=src, dst_ref=home_ref.at[slot],
                send_sem=send.at[20 + r], recv_sem=recv.at[20 + slot],
                device_id=(target, target_c), device_id_type=MESH,
            ).start()

    to_core.wait_recv()
    plane_in[c] = vec_ref[...] + core_in[...]
    across = []
    for n, peer in enumerate((peer_x, peer_y, peer_d)):
        across.append(copy(plane_in.at[c], plane_in.at[c], 5 + n, (me, peer)))

    for q in order:
        hops[q].wait_recv()
        index = y if q < 2 else x
        total = block(q, c) + first(q, index) + got[q].astype(f32)
        line_out[q] = total.astype(bf16)
        if q == order[0]:
            for item in across:
                item.start()
        target = 4 * k + q
        here = target == me

        @pl.when(here)
        def _():
            line_in[z] = line_out[q]

        @pl.when(jnp.logical_not(here))
        def _():
            pltpu.make_async_remote_copy(
                src_ref=line_out.at[q], dst_ref=line_in.at[z],
                send_sem=send.at[8 + q], recv_sem=recv.at[8 + z],
                device_id=(target, c), device_id_type=MESH,
            ).start()

    for item in across:
        item.wait_recv()
    for n in range(4):
        mods_ref[z, n] = plane_in[n, :HALF_ROWS, :].astype(bf16).astype(f32)
    bias_in[z] = (plane_in[0, HALF_ROWS:, :] + plane_in[1, HALF_ROWS:, :]) + (
        plane_in[2, HALF_ROWS:, :] + plane_in[3, HALF_ROWS:, :]
    )
    far = []
    for n in range(1, 4):
        other = ((z + n) % 4) * 2 + k
        far.append(copy(mods_ref.at[z], mods_ref.at[z], 14 + n, (other, c)))
        far.append(copy(bias_in.at[z], bias_in.at[z], 22 + n, (other, c)))

    for item in far:
        item.start()
    owner_core = me // 4
    total = None
    for n in range(4):
        here = (z == n) & (k == owner_core)

        @pl.when(jnp.logical_not(here))
        def _():
            pltpu.make_async_remote_copy(
                src_ref=line_in.at[n], dst_ref=line_in.at[n],
                send_sem=send.at[8 + n], recv_sem=recv.at[8 + n],
                device_id=(partner, c), device_id_type=MESH,
            ).wait_recv()

    for n in range(4):
        value = line_in[n].astype(f32)
        total = value if total is None else total + value
    shared[c] = total.astype(bf16)
    spread = []
    for n, peer in enumerate((peer_x, peer_y, peer_d)):
        spread.append(copy(shared.at[c], shared.at[c], 12 + n, (me, peer)))
    for item in spread:
        item.start()
    for item in far:
        item.wait_recv()
    bias_ref[...] = (bias_in[0] + bias_in[1]) + (bias_in[2] + bias_in[3])

    act_out[...] = jnp.zeros(COND, f32)
    d_act = None
    for p in range(6):
        lhs = jnp.concatenate(
            [mods_ref[n, m, p : p + 1, :] for n in range(4) for m in range(4)], 0
        ).astype(bf16)
        term = contract(lhs, ada_ref[:, p * D : (p + 1) * D], 1, 1)
        d_act = term if d_act is None else d_act + term
    for n in range(4):
        for side in range(2):
            for m in range(2):
                at = n * 4 + m * 2 + side
                act_out[n * 2 + side, m : m + 1, :rows] = d_act[at : at + 1, :]
    cond_ref[me] = act_out[me]
    acts = []
    for n in range(1, 8):
        other = (me + n) % 8
        acts.append(copy(act_out.at[other], cond_ref.at[me], 25 + n, (other, c)))
    for item in spread:
        item.wait_recv()
    for item in acts:
        item.start()
    for j in range(3):
        gq_ref[:, j * D : (j + 1) * D] = shared[j].astype(f32)
    go_ref[...] = shared[3].astype(f32)

    for slot in range(2):
        here = (slot * 2 + k == c) & (y == k)

        @pl.when(jnp.logical_not(here))
        def _():
            pltpu.make_async_remote_copy(
                src_ref=home_ref.at[slot], dst_ref=home_ref.at[slot],
                send_sem=send.at[20 + slot], recv_sem=recv.at[20 + slot],
                device_id=(partner, c), device_id_type=MESH,
            ).wait_recv()

        tokens_ref[slot] = home_ref[slot].astype(f32)

    for item in acts:
        item.wait_recv()

    for r in range(2):
        here = (x == k) & (2 * k + (y + r) % 2 == c)

        @pl.when(jnp.logical_not(here))
        def _():
            pltpu.make_async_remote_copy(
                src_ref=gl_ref.at[pl.ds(r * length, length), :], dst_ref=home_ref.at[0],
                send_sem=send.at[20 + r], recv_sem=recv.at[20],
                device_id=(partner, c), device_id_type=MESH,
            ).wait_send()

    for q in range(4):
        here = 4 * k + q == me

        @pl.when(jnp.logical_not(here))
        def _():
            pltpu.make_async_remote_copy(
                src_ref=line_out.at[q], dst_ref=line_in.at[q],
                send_sem=send.at[8 + q], recv_sem=recv.at[8],
                device_id=(partner, c), device_id_type=MESH,
            ).wait_send()

    for item in started + [hops[q] for q in order] + across + far + spread + acts:
        item.wait_send()


def finish(chip, first_x, first_y, tokens, vector, ada_w):
    rows = chip.shape[0] // 4
    length = tokens.shape[0] // 2
    vmem = pl.BlockSpec(memory_space=pltpu.VMEM)
    piece = (4, rows, D)
    return pl.pallas_call(
        finish_kernel,
        in_specs=[vmem] * 6,
        out_specs=[vmem] * 6,
        out_shape=[
            jax.ShapeDtypeStruct((rows, 3 * D), f32),
            jax.ShapeDtypeStruct((rows, D), f32),
            jax.ShapeDtypeStruct((2, length, D), f32),
            jax.ShapeDtypeStruct((4, 4, HALF_ROWS, D), f32),
            jax.ShapeDtypeStruct((HALF_ROWS, D), f32),
            jax.ShapeDtypeStruct(COND, f32),
        ],
        scratch_shapes=[pltpu.VMEM(piece, bf16)] * 5
        + [
            pltpu.VMEM((2, length, D), bf16),
            pltpu.VMEM((2 * HALF_ROWS, D), f32),
            pltpu.VMEM((4, 2 * HALF_ROWS, D), f32),
            pltpu.VMEM((4, HALF_ROWS, D), f32),
            pltpu.VMEM(COND, f32),
            pltpu.SemaphoreType.DMA((33,)),
            pltpu.SemaphoreType.DMA((33,)),
        ],
        compiler_params=pltpu.CompilerParams(
            collective_id=1, has_side_effects=True, vmem_limit_bytes=40 * 2**20
        ),
        name="finish",
    )(chip, first_x, first_y, tokens, vector, ada_w)


COND = (8, 8, 256)


def greet(z, k, c):
    barrier = pltpu.get_barrier_semaphore()
    devices = [(z * 2 + (k + a) % 2, (c + b) % 4) for a in range(2) for b in range(4) if a or b]
    devices += [(((z + a) % 4) * 2 + (k + b) % 2, c) for a in range(1, 4) for b in range(2)]
    for device in devices:
        pl.semaphore_signal(barrier, inc=1, device_id=device, device_id_type=MESH)
    pl.semaphore_wait(barrier, len(devices))


def begin_kernel(
    qkv_ref, out_ref, x_ref, up_ref, cond_ref, bias_ref, ada_ref, own_ref,
    qkv_all, out_all, x_all, up_all, cond_all, bias_all, mod_ref,
    part, part_in, send, recv,
):
    rows = qkv_ref.shape[0]
    me, c = lax.axis_index("dp"), lax.axis_index("ctx")
    z, k = me // 2, me % 2
    y, x = c // 2, c % 2
    peer_x, peer_y, peer_d = y * 2 + 1 - x, (1 - y) * 2 + x, (1 - y) * 2 + 1 - x
    partner = me + 1 - 2 * k
    greet(z, k, c)

    def copy(src, dst, index, device):
        return pltpu.make_async_remote_copy(
            src_ref=src, dst_ref=dst, send_sem=send.at[index], recv_sem=recv.at[index],
            device_id=device, device_id_type=MESH,
        )

    def band(owner):
        return pl.ds(pl.multiple_of(owner * rows, 16), rows)

    def columns(j):
        return pl.ds(pl.multiple_of(j * D, D), D)

    def push(j, owner, index, device, own=False):
        @pl.when(j < 3)
        def _():
            place = qkv_all.at[band(owner), columns(j)]
            copy(qkv_ref.at[:, columns(j)] if own else place, place, index, device).start()

        @pl.when(j == 3)
        def _():
            place = out_all.at[band(owner), :]
            copy(out_ref if own else place, place, index, device).start()

    def piece(index):
        place = out_all.at[band(me), :]
        return copy(out_ref, place, index, (partner, c))

    for r in range(1, 4):
        push(c, me, r - 1, (((z + r) % 4) * 2 + k, c), own=True)

    small = []
    for r in range(1, 8):
        other = (me + r) % 8
        small.append(copy(cond_ref.at[other], cond_all.at[me], 25 + r, (other, c)))
        small.append(copy(bias_ref, bias_all.at[me], 32 + r, (other, c)))
    for item in small:
        item.start()

    for r in range(2):
        micro = (c + r) % 2
        target, target_c = z * 2 + y, micro * 2 + k
        here = (y == k) & (target_c == c)

        @pl.when(here)
        def _():
            x_all[r] = x_ref[micro]
            up_all[r] = up_ref[micro]

        @pl.when(jnp.logical_not(here))
        def _():
            copy(x_ref.at[micro], x_all.at[r], 47 + r, (target, target_c)).start()
            copy(up_ref.at[micro], up_all.at[r], 51 + r, (target, target_c)).start()

    mine = [
        pltpu.make_async_copy(qkv_ref, qkv_all.at[band(me), :], send.at[49]),
        pltpu.make_async_copy(out_ref, out_all.at[band(me), :], send.at[50]),
    ]
    across = [
        copy(qkv_ref, qkv_all.at[band(me), :], 12, (partner, c)),
        copy(out_ref, out_all.at[band(me), :], 13, (partner, c)),
    ]
    for item in across + mine:
        item.start()

    cond_all[me] = cond_ref[me]
    bias_all[me] = bias_ref[...]
    for item in small[0::2]:
        item.wait_recv()
    acts = []
    for plane in range(4):
        value = cond_all[plane * 2 + x]
        value = jnp.where(y == 0, value[0:1, :], value[1:2, :])
        acts.append(value / (1.0 + jnp.exp(-value)))
    act = jnp.concatenate(acts + acts, 0)[:, :rows].astype(bf16)
    terms = contract(act, ada_ref[...], 1, 0)
    for plane in range(4):
        part[plane] = terms[plane : plane + 1, :] + own_ref[...]

    def piece_from(index):
        piece(index).wait_recv()

    def owner(r):
        return ((z + 4 - r) % 4) * 2 + k

    for r in range(1, 4):
        piece_from(r - 1)
        push(c, owner(r), 2 + r, (me, peer_x))
        push(c, owner(r), 5 + r, (me, peer_y))
        push(c, owner(r), 13 + r, (partner, c))
        if r == 1:
            sums = []
            for n in range(1, 8):
                other = (me + n) % 8
                sums.append(copy(part.at[other // 2], part_in.at[me], 39 + n, (other, c)))
            for item in sums:
                item.start()
            part_in[me] = part[z]

    for r in range(1, 4):
        piece_from(2 + r)
        if r < 3:
            push(peer_x, owner(r), 8 + r, (me, peer_y))
        push(peer_x, owner(r), 16 + r, (partner, c))
        piece_from(5 + r)
        if r == 3:
            push(peer_y, owner(r), 8 + r, (me, peer_x))
        push(peer_y, owner(r), 19 + r, (partner, c))

    for item in sums:
        item.wait_recv()
    total = part_in[0]
    for n in range(1, 8):
        total = total + part_in[n]
    mod_ref[...] = total

    for r in range(1, 4):
        piece_from(8 + r)
        push(peer_d, owner(r), 22 + r, (partner, c))

    for item in small[1::2] + across:
        item.wait_recv()
    for index in range(14, 26):
        piece_from(index)
    for r in range(2):
        here = (2 * k + (y + r) % 2 == c) & (x == k)

        @pl.when(jnp.logical_not(here))
        def _():
            copy(x_ref.at[0], x_all.at[r], 47 + r, (partner, c)).wait_recv()
            copy(up_ref.at[0], up_all.at[r], 51 + r, (partner, c)).wait_recv()

    for r in range(2):
        micro = (c + r) % 2
        here = (y == k) & (micro * 2 + k == c)

        @pl.when(jnp.logical_not(here))
        def _():
            copy(x_ref.at[0], x_all.at[r], 47 + r, (partner, c)).wait_send()
            copy(up_ref.at[0], up_all.at[r], 51 + r, (partner, c)).wait_send()

    for index in list(range(12)) + list(range(14, 26)):
        piece(index).wait_send()
    for item in small + across + sums:
        item.wait_send()
    for item in mine:
        item.wait()


def begin(qkv_w, out_w, tokens, upstream, cond, bias, ada_w, own_bias):
    rows = qkv_w.shape[0]
    vmem = pl.BlockSpec(memory_space=pltpu.VMEM)
    hbm = pl.BlockSpec(memory_space=pl.ANY)
    return pl.pallas_call(
        begin_kernel,
        in_specs=[vmem] * 8,
        out_specs=[hbm, hbm, vmem, vmem, vmem, vmem, vmem],
        out_shape=[
            jax.ShapeDtypeStruct((8 * rows, 3 * D), bf16),
            jax.ShapeDtypeStruct((8 * rows, D), bf16),
            jax.ShapeDtypeStruct(tokens.shape, bf16),
            jax.ShapeDtypeStruct(tokens.shape, bf16),
            jax.ShapeDtypeStruct(COND, f32),
            jax.ShapeDtypeStruct((8, 1, D), f32),
            jax.ShapeDtypeStruct((1, 6 * D), f32),
        ],
        scratch_shapes=[
            pltpu.VMEM((4, 1, 6 * D), f32),
            pltpu.VMEM((8, 1, 6 * D), f32),
            pltpu.SemaphoreType.DMA((53,)),
            pltpu.SemaphoreType.DMA((53,)),
        ],
        compiler_params=pltpu.CompilerParams(
            collective_id=2, has_side_effects=True, vmem_limit_bytes=32 * 2**20
        ),
        name="begin",
    )(qkv_w, out_w, tokens, upstream, cond, bias, ada_w, own_bias)


def local(
    latents,
    condition,
    cotangent,
    ada_weight,
    ada_bias,
    qkv_weight,
    query_bias,
    value_bias,
    out_weight,
    out_bias,
    fc1_weight,
    fc1_bias,
    fc2_weight,
    fc2_bias,
    *,
    dp,
    ctx,
):
    micro, _, length, _ = latents.shape
    planes = dp // 2
    rows = D // dp
    fast = ctx == 4 and dp == 8 and micro == 2
    per_latent = ctx // micro
    me_dp = lax.axis_index("dp")
    me_ctx = lax.axis_index("ctx")
    core = me_dp % 2
    moves = move_maps(dp, ctx, micro)
    peers = peer_maps(dp, ctx, micro)
    my_latent = me_ctx * 2 // per_latent

    def bring(value):
        came = []
        for r in range(micro):
            block = lax.dynamic_index_in_dim(value, (me_ctx + r) % micro, 0, keepdims=False)[0]
            came.append(lax.ppermute(block, BOTH, moves[r]))
        return jnp.concatenate(came, 0)

    def send_home(value):
        came = jnp.stack(
            [
                lax.ppermute(value[r * length : (r + 1) * length], BOTH, inverse(moves[r]))
                for r in range(micro)
            ]
        )
        return jnp.stack(
            [
                lax.dynamic_index_in_dim(came, (m - me_ctx) % micro, 0, keepdims=False)
                for m in range(micro)
            ]
        )[:, None]

    own_bias = lax.dynamic_update_slice_in_dim(
        jnp.zeros((6 * D,), f32), ada_bias.astype(f32), me_dp * (6 * D // dp), 0
    )
    small = jnp.concatenate([query_bias, value_bias, out_bias, fc1_bias, fc2_bias])
    if fast:
        cond = condition[:, 0].reshape(micro, dp, rows).transpose(1, 0, 2).astype(f32)
        cond = jnp.pad(cond, ((0, 0), (0, COND[1] - micro), (0, COND[2] - rows)))
        qkv_w, out_w, x_low, upstream_low, conds, bias_all, modul = begin(
            qkv_weight,
            out_weight,
            latents[:, 0],
            cotangent[:, 0],
            cond,
            small.astype(f32)[None],
            ada_weight,
            own_bias[None],
        )
        x_low = x_low.reshape(micro * length, D)
        upstream_low = upstream_low.reshape(micro * length, D)
        act_rows = jax.nn.silu(conds[:, :micro, :rows]).astype(bf16)
        act_rows = act_rows.reshape(planes, 2, micro, rows).transpose(0, 2, 1, 3)
        bias_all = bias_all[:, 0]
        modul = modul[0]
    else:
        qkv_w = lax.all_gather(qkv_weight, "dp", axis=0, tiled=True)
        out_w = lax.all_gather(out_weight, "dp", axis=0, tiled=True)
        x_low = bring(latents)
        upstream_low = bring(cotangent)
        small = jnp.concatenate([condition[:, 0].reshape(micro * D), small])
        small_all = gather_small(small, "dp", dp)
        cond_all = small_all[:, : micro * D].reshape(dp, micro, D)
        bias_all = small_all[:, micro * D :].astype(f32)
        act_rows = jax.nn.silu(
            lax.dynamic_slice_in_dim(cond_all, me_dp * rows, rows, 2).astype(f32)
        ).astype(bf16)
        act_rows = act_rows.reshape(planes, 2, micro, rows).transpose(0, 2, 1, 3)
        act_mine = lax.dynamic_index_in_dim(
            act_rows.reshape(planes, micro * 2, rows), my_latent, 1, keepdims=False
        )
        partial_mod = jnp.dot(act_mine, ada_weight, preferred_element_type=f32) + own_bias
        modul = 0.0
        for r in range(dp):
            row = lax.dynamic_index_in_dim(partial_mod, (me_dp + r) % dp // 2, 0, keepdims=False)
            modul = modul + (ring(row, "dp", dp, r) if r else row)
    fc1_w = lax.all_gather(fc1_weight, "dp", axis=0, tiled=True)
    fc2_w = lax.all_gather(fc2_weight, "dp", axis=0, tiled=True)
    query_b = bias_all[:, :rows].reshape(D)
    value_b = bias_all[:, rows : 2 * rows].reshape(D)
    out_b = bias_all[:, 2 * rows : 3 * rows].reshape(D)
    fc1_b = bias_all[:, 3 * rows : 3 * rows + FF // dp].reshape(FF)
    fc2_b = bias_all[:, 3 * rows + FF // dp :].reshape(D)
    shift_one, scale_one, gate_one, shift_two, scale_two, gate_two = [
        modul[part * D : (part + 1) * D] for part in range(6)
    ]

    inputs = x_low.astype(f32)
    normed_one, inverse_one = norm_rows(inputs)
    mixed_one = (normed_one * (1.0 + scale_one) + shift_one).astype(bf16)
    qkv_bias = jnp.concatenate([query_b, jnp.zeros((D,), f32), value_b])
    qkv = (contract(qkv_w, mixed_one, 0, 1) + qkv_bias[:, None]).astype(bf16)
    others = [lax.ppermute(qkv[D:], BOTH, peer) for peer in peers]
    attended, lse = attend(qkv, others)
    branch_one = contract(attended, out_w, 0, 0) + out_b
    middle = inputs + gate_one * branch_one
    normed_two, inverse_two = norm_rows(middle)
    mixed_two = (normed_two * (1.0 + scale_two) + shift_two).astype(bf16)
    pre_act = jnp.dot(mixed_two, fc1_w, preferred_element_type=f32) + fc1_b
    hidden_low, slope = gelu_pair(pre_act)
    branch_two = jnp.dot(hidden_low, fc2_w, preferred_element_type=f32) + fc2_b
    block_out = send_home((middle + gate_two * branch_two).astype(bf16))

    side_y, side_x = me_ctx // 2, me_ctx % 2

    def halves(values):
        width = values.shape[1] // 2
        return (
            lax.dynamic_slice_in_dim(values, core * width, width, 1),
            lax.dynamic_slice_in_dim(values, (1 - core) * width, width, 1),
        )

    def give(values, grads, dim):
        return swap_cores(contract(halves(values)[1], grads, 0, dim).astype(bf16), dp)

    def keep(values, grads, dim, came):
        return (contract(halves(values)[0], grads, 0, dim) + came.astype(f32)).astype(bf16)

    def hop(value, bit):
        return lax.ppermute(value, "ctx", [(i, i ^ bit) for i in range(4)])

    def plane_give(pick):
        along_x = jnp.stack([pick(y * 2 + 1 - side_x, 0) for y in range(2)])
        along_y = jnp.stack([pick((1 - side_y) * 2 + x, 1) for x in range(2)])
        return along_x, along_y

    def plane_first(given):
        return hop(given[0], 1), hop(given[1], 2)

    def plane_second(pick, came):
        def term(half, index, j):
            value = lax.dynamic_index_in_dim(came[half], index, 0, keepdims=False)
            return pick(j, half).astype(f32) + value.astype(f32)

        along_y = hop(term(0, 1 - side_y, (1 - side_y) * 2 + side_x).astype(bf16), 2)
        along_x = hop(term(1, 1 - side_x, side_y * 2 + 1 - side_x).astype(bf16), 1)
        return along_y, along_x

    def plane_last(pick, came, more):
        total = []
        for half, index in ((0, side_y), (1, side_x)):
            value = lax.dynamic_index_in_dim(came[half], index, 0, keepdims=False)
            total.append(
                pick(me_ctx, half).astype(f32) + value.astype(f32) + more[half].astype(f32)
            )
        return jnp.concatenate(total, 0).astype(bf16)

    def line_moves(block):
        moved = []
        for r in range(4):
            piece = lax.dynamic_index_in_dim(block, (me_dp // 2 + r) % 4, 0, keepdims=False)
            pairs = [(i, 4 * (i % 2) + (i // 2 + r) % 4) for i in range(8)]
            moved.append(lax.ppermute(piece, "dp", pairs))
        return moved

    def total_of(values):
        return sum(v.astype(f32) for v in values).astype(bf16)

    def share(block):
        return [block] + [hop(block, r) for r in range(1, 4)]

    def in_order(came):
        stack = jnp.stack(came)
        return [
            lax.dynamic_index_in_dim(stack, me_ctx ^ j, 0, keepdims=False).astype(f32)
            for j in range(4)
        ]

    def row_pick(chip):
        return lambda j, half: lax.dynamic_slice(
            chip, (half * 2 * rows, j * D), (2 * rows, D)
        ).reshape(2, rows, D)

    def slow_sum(values, grads, dim):
        total = contract(values, grads, 0, dim).astype(bf16)
        total = lax.psum_scatter(total, "dp", scatter_dimension=0, tiled=True)
        return lax.psum(total, "ctx").astype(f32)

    def tie(*values):
        return lax.optimization_barrier(values)

    upstream = upstream_low.astype(f32)
    d_gate_two = jnp.sum(branch_two * upstream, 0)
    d_branch_two = (gate_two * upstream).astype(bf16)
    sum_fc2_b = jnp.sum(d_branch_two.astype(f32), 0)
    if fast:
        came_fc2 = give(hidden_low, d_branch_two, 0)
    d_hidden = contract(d_branch_two, fc2_w, 1, 1)
    d_pre = (d_hidden * slope.astype(f32)).astype(bf16)
    sum_fc1_b = jnp.sum(d_pre.astype(f32), 0)
    if fast:
        came_fc2, d_pre = tie(came_fc2, d_pre)
        chip_fc2 = keep(hidden_low, d_branch_two, 0, came_fc2).reshape(4, 4, rows, D)

        def pick_fc2(j, half):
            return lax.dynamic_index_in_dim(
                chip_fc2[2 * half : 2 * half + 2], j, 1, keepdims=False
            )

        given, d_pre = tie(plane_give(pick_fc2), d_pre)
        first_fc2 = plane_first(given)
        came_fc1 = give(mixed_two, d_pre, 0)
    d_mixed_two = contract(d_pre, fc1_w, 1, 1)
    d_shift_two = jnp.sum(d_mixed_two, 0)
    d_scale_two = jnp.sum(d_mixed_two * normed_two, 0)
    if fast:
        came_fc1, first_fc2, d_mixed_two = tie(came_fc1, first_fc2, d_mixed_two)
        second_fc2 = plane_second(pick_fc2, first_fc2)
        chip_fc1 = keep(mixed_two, d_pre, 0, came_fc1)
        pick_fc1 = row_pick(chip_fc1)
        given, d_mixed_two = tie(plane_give(pick_fc1), d_mixed_two)
        first_fc1 = plane_first(given)
    d_middle = upstream + norm_back(d_mixed_two * (1.0 + scale_two), normed_two, inverse_two)
    d_gate_one = jnp.sum(branch_one * d_middle, 0)
    d_branch_one = (gate_one * d_middle).astype(bf16)
    sum_out_b = jnp.sum(d_branch_one.astype(f32), 0)
    d_attended = contract(out_w, d_branch_one, 1, 1).astype(bf16)
    if fast:
        came_out = give(attended.T, d_branch_one, 0)
        plane_fc2 = plane_last(pick_fc2, first_fc2, second_fc2)

    calls = (2, 2, 4)
    d_query, d_key, d_value = [], [], []
    pending = None

    def settle(result):
        d_own, moved = result
        total = d_own.astype(f32)
        for value in moved:
            total = total + value.astype(f32)
        total = total.astype(bf16)
        d_key.append(total[0])
        d_value.append(total[1])

    for call, count in enumerate(calls):
        d_q, d_own, *d_others = attend_back(
            qkv, others, attended, d_attended, lse, sum(calls[:call]), count
        )
        if fast and call == 0:
            d_q, first_fc1 = tie(d_q, first_fc1)
            second_fc1 = plane_second(pick_fc1, first_fc1)
            chip_out = keep(attended.T, d_branch_one, 0, came_out)
            chip_out, d_attended = tie(chip_out, d_attended)
        elif fast and call == 1:
            d_q, second_fc1 = tie(d_q, second_fc1)
            plane_fc = jnp.stack([plane_fc2, plane_last(pick_fc1, first_fc1, second_fc1)], 1)
            plane_fc, d_attended = tie(plane_fc, d_attended)
            moved_fc = line_moves(plane_fc)
        elif fast and call == 2:
            d_q, moved_fc = tie(d_q, moved_fc)
            moved_fc = total_of(moved_fc)
            shared_fc = share(moved_fc)
        d_query.append(d_q)
        if call < len(calls) - 1:
            d_others, d_attended = tie(d_others, d_attended)
        moved = [lax.ppermute(value, BOTH, inverse(peer)) for peer, value in zip(peers, d_others)]
        if pending is not None:
            settle(pending)
        pending = (d_own, moved)
    settle(pending)
    d_qkv = jnp.concatenate(d_query + d_key + d_value, 0)
    sum_qkv_b = jnp.sum(d_qkv.astype(f32), 1)
    if fast:
        came_qkv = give(mixed_one, d_qkv, 1)
        chip_qkv = keep(mixed_one, d_qkv, 1, came_qkv)
        chip_attn = jnp.concatenate([chip_qkv, chip_out], 1)
        given, d_qkv = tie(plane_give(row_pick(chip_attn)), d_qkv)
        first_attn = plane_first(given)
    d_mixed_one = contract(d_qkv, qkv_w, 0, 1)
    d_shift_one = jnp.sum(d_mixed_one, 0)
    d_scale_one = jnp.sum(d_mixed_one * normed_one, 0)
    d_inputs = d_middle + norm_back(d_mixed_one * (1.0 + scale_one), normed_one, inverse_one)
    mod_sums = jnp.concatenate(
        [d_shift_one, d_scale_one, d_gate_one, d_shift_two, d_scale_two, d_gate_two]
    )
    bias_sums = jnp.concatenate(
        [sum_qkv_b[:D], sum_qkv_b[2 * D :], sum_out_b, sum_fc1_b, sum_fc2_b]
    )
    lats = micro * 2

    if fast:
        vector = jnp.concatenate(
            [mod_sums, jnp.zeros((2 * D,), f32), bias_sums]
        ).reshape(2 * HALF_ROWS, D)
        grad_qkv_w, grad_out_w, home, mods, bias_sums, d_cond = finish(
            chip_attn,
            first_attn[0].reshape(2, 2 * rows, D),
            first_attn[1].reshape(2, 2 * rows, D),
            d_inputs.astype(bf16),
            vector,
            ada_weight,
        )
        grad_latents = home[:, None]
        flat_modul = mods[:, :, :6].astype(bf16).reshape(planes * lats, 6 * D)
        d_cond = d_cond[:, :micro, :rows]
        bias_sums = bias_sums.reshape(-1)
        shared_fc = in_order(shared_fc)
        grad_fc2_w = jnp.concatenate([v[0] for v in shared_fc], 0)
        grad_fc1_w = jnp.concatenate([v[1] for v in shared_fc], 1)
    else:
        grad_fc2_w = slow_sum(hidden_low, d_branch_two, 0)
        grad_fc1_w = slow_sum(mixed_two, d_pre, 0)
        grad_out_w = slow_sum(attended.T, d_branch_one, 0)
        grad_qkv_w = slow_sum(mixed_one, d_qkv, 1)
        grad_latents = send_home(d_inputs.astype(bf16)).astype(f32)
        vector = jnp.concatenate([mod_sums, bias_sums])
        vector = vector + swap_cores(vector, dp)
        chips = gather_small(vector, "ctx", ctx)
        d_mods = jnp.sum(chips[:, : 6 * D].reshape(lats, ctx // lats, 6 * D), 1)
        packed = jnp.concatenate(
            [d_mods.reshape(lats * 6 * D), jnp.sum(chips[:, 6 * D :], 0)]
        ).astype(bf16)
        packed = gather_small(packed, "dp", dp, 2)
        flat_modul = packed[:, : lats * 6 * D].reshape(planes * lats, 6 * D)
        bias_sums = jnp.sum(packed[:, lats * 6 * D :].astype(f32), 0)

    def owned(start, width):
        return lax.dynamic_slice_in_dim(bias_sums, start + me_dp * (width // dp), width // dp)

    grad_query_b = owned(0, D)
    grad_value_b = owned(D, D)
    grad_out_b = owned(2 * D, D)
    grad_fc1_b = owned(3 * D, FF)
    grad_fc2_b = owned(3 * D + FF, D)
    grad_ada_w = contract(act_rows.reshape(planes * lats, rows), flat_modul, 0, 0)
    grad_ada_b = lax.dynamic_slice_in_dim(
        jnp.sum(flat_modul.astype(f32), 0), me_dp * (6 * D // dp), 6 * D // dp
    )
    if not fast:
        d_act = contract(flat_modul, ada_weight, 1, 1)
        d_act = d_act.reshape(planes, micro, 2, rows).transpose(0, 2, 1, 3)
        d_act = d_act.reshape(dp, micro, rows)
        came = []
        for r in range(dp):
            piece = lax.dynamic_index_in_dim(d_act, (me_dp + r) % dp, 0, keepdims=False)
            came.append(ring(piece, "dp", dp, r) if r else piece)
        back = jnp.stack(came[::-1])
        d_cond = lax.dynamic_slice_in_dim(jnp.concatenate([back, back]), dp - 1 - me_dp, dp)
    d_cond = d_cond.transpose(1, 0, 2).reshape(micro, D)
    cond_f = condition[:, 0].astype(f32)
    gate = 1.0 / (1.0 + jnp.exp(-cond_f))
    grad_condition = (d_cond * gate * (1.0 + cond_f * (1.0 - gate)))[:, None]

    return (
        block_out,
        grad_latents,
        grad_condition,
        grad_ada_w,
        grad_ada_b,
        grad_qkv_w,
        grad_query_b,
        grad_value_b,
        grad_out_w,
        grad_out_b,
        grad_fc1_w,
        grad_fc1_b,
        grad_fc2_w,
        grad_fc2_b,
    )


def solution(mesh):
    token = P(None, "dp", "ctx", None)
    line = P(None, "dp", None)
    wide, flat = P("dp", None), P("dp")
    weights = (wide, flat, wide, flat, flat, wide, flat, wide, flat, wide, flat)
    return jax.shard_map(
        partial(local, dp=mesh.shape["dp"], ctx=mesh.shape["ctx"]),
        mesh=mesh,
        in_specs=(token, line, token) + weights,
        out_specs=(token, token, line) + weights,
        check_vma=False,
    )
```
